32 devices in a mesh: tm: 8 (over y, x, core), cell: 4 (over z).
Axes of the slice: x: 2, y: 2, z: 4, core: 2. Of those that a mesh axis runs over, the one named last changes fastest.
Arguments:
- anomalies: bfloat16 [24, 2, 8192, 256], P('tm', None, 'cell'), may hold values from -6 to 6
- obs_cells: int32 [24, 128], P('tm', 'cell'), may hold values from 0 to 8191, as said below
- obs_counts: int32 [24, 4], P('tm', 'cell'), may hold values from 16 to 32
- obs_precision: float32 [24, 128], P('tm', 'cell'), may hold values from 0.1 to 1
- inflation: float32 [24], P('tm'), may hold values from 1 to 1.12
Outputs:
- smoothed: bfloat16 [24, 2, 8192, 256], P('tm', None, 'cell')
The draws below stay inside these ranges and needn't reach their ends.
Inputs may be any that keep to these rules, and one draw needn't show every extreme that they name: `obs_cells`: slot k of a window names a cell of the block of 2048 cells that starts at (k // 32) * 2048; two slots may name the same cell.
All inputs are finite; a program needn't handle non-finite values.
Results may differ from the reference program's by a relative error of at most 0.017.
Values may be sent and summed in bfloat16 or wider, within the bound.
A program may use at most 128 MiB of HBM per device.

```python
import math
import jax
import jax.numpy as jnp
from jax import lax

M = 256
CELL_DEV = 2048
OBS_DEV = 32
WINDOWS = 24
CELLS = 8192
OBS = 128
N_CELL = 4


def draw_obs_cells(key, part):
    block = jnp.arange(OBS, dtype=jnp.int32) // OBS_DEV
    offsets = jax.random.randint(key, (WINDOWS, OBS), 0, CELL_DEV, dtype=jnp.int32)
    return offsets + block[None, :] * CELL_DEV


def set_ends(entries, rng, low, top_value):
    longest = entries.shape.index(max(entries.shape))
    spots = []
    for shift in (0, 1):
        where = [jax.random.randint(jax.random.fold_in(rng, axis), (), 0, length) for axis, length in enumerate(entries.shape)]
        where[longest] = (where[longest] + shift) % entries.shape[longest]
        spots.append(tuple(where))
    return entries.at[spots[0]].set(low).at[spots[1]].set(top_value)


def level_of(stream_key, dims, pieces, smallest, high):
    gain = 1.0
    for position, blocks in pieces:
        heights = jax.random.uniform(jax.random.fold_in(jax.random.fold_in(stream_key, 6), position), (blocks,), jnp.float32, smallest / len(pieces), high / len(pieces))
        gain = gain * jnp.repeat(jnp.exp(heights), dims[position] // blocks).reshape((-1,) + (1,) * (len(dims) - 1 - position))
    return gain


def normal_values(key, shape, deviation, reach, shards=(), kind=jnp.bfloat16):
    values = deviation * jax.random.normal(key, shape, jnp.float32)
    if shards:
        values = values * level_of(key, shape, shards, -0.22, 0.18)
    return jnp.clip(values, -reach, reach).astype(kind)


def setup_inputs(seed: int = 0) -> dict:
    streams_of = jax.random.split(jax.random.key(seed), 6)
    anomalies = normal_values(streams_of[0], (WINDOWS, 2, CELLS, M), 1.0, 6.0, ((0, 8), (2, 4)))
    obs_cells = draw_obs_cells(jax.random.fold_in(streams_of[5], 71), 0)
    obs_counts = set_ends(jax.random.randint(streams_of[2], (WINDOWS, N_CELL), OBS_DEV // 2, OBS_DEV + 1), jax.random.fold_in(streams_of[2], 1), OBS_DEV // 2, OBS_DEV).astype(jnp.int32)
    obs_precision = jnp.clip(jnp.exp(math.log(1.0) - 2.3025851 * jax.random.uniform(streams_of[3], (WINDOWS, OBS), jnp.float32) ** level_of(streams_of[3], (WINDOWS, OBS), ((0, 8), (1, 4)), -0.2, 0.2)), 0.1, 1.0)
    inflation = jnp.clip(jnp.exp(math.log(1.12) - 0.11332869 * jax.random.uniform(streams_of[4], (WINDOWS,), jnp.float32) ** level_of(streams_of[4], (WINDOWS,), ((0, 8),), -0.2, 0.2)), 1.0, 1.12)
    return {"anomalies": anomalies, "obs_cells": obs_cells, "obs_counts": obs_counts, "obs_precision": obs_precision, "inflation": inflation}


def one_transform(packed):
    field, cells, counts_row, precision, rho = packed
    picked = field[0][cells].astype(jnp.float32)
    slot = jnp.arange(OBS) % OBS_DEV
    block = jnp.arange(OBS) // OBS_DEV
    live = slot < counts_row[block]
    weights = jnp.where(live, precision, jnp.float32(0.0))
    weighted = picked * weights[:, None]
    gram = jnp.dot(weighted.T.astype(jnp.float32), picked.astype(jnp.float32), precision=lax.Precision.HIGHEST, preferred_element_type=jnp.float32)
    unit_matrix = jnp.eye(M, dtype=jnp.float32)
    system = (M - 1.0) * unit_matrix + gram
    factor = jnp.linalg.cholesky(system)
    inverse = jax.scipy.linalg.solve_triangular(factor, unit_matrix, lower=True)
    return rho * jnp.sqrt(jnp.float32(M - 1.0)) * inverse.T

def reference(anomalies, obs_cells, obs_counts, obs_precision, inflation):
    transforms = lax.map(one_transform, (anomalies, obs_cells, obs_counts, obs_precision, inflation))

    def backward(carried, current):
        product = jnp.dot(current.astype(jnp.float32), carried.astype(jnp.float32), precision=lax.Precision.HIGHEST, preferred_element_type=jnp.float32)
        return (product, product)
    unit_matrix = jnp.eye(M, dtype=jnp.float32)
    _, suffixes = lax.scan(backward, unit_matrix, transforms, reverse=True)
    weights = suffixes.astype(jnp.bfloat16)

    def apply_window(packed):
        field, weight_matrix = packed
        flat = field.reshape(2 * CELLS, M)
        result = jnp.dot(flat.astype(jnp.float32), weight_matrix.astype(jnp.float32), preferred_element_type=jnp.float32)
        return result.astype(jnp.bfloat16).reshape(2, CELLS, M)
    return lax.map(apply_window, (anomalies, weights))
```

```python
import jax
import jax.numpy as jnp
from jax import lax
from jax.experimental import pallas as pl
from jax.experimental.pallas import tpu as pltpu
from jax.sharding import PartitionSpec as P

F32 = jnp.float32
BF16 = jnp.bfloat16
SPREAD_GAIN = 1.4
SETTLED = 4e-4
MIB = 1 << 20


def dot_any(left, right, dims):
    return lax.dot_general(left, right, (dims, ((), ())), preferred_element_type=F32)


def halves(value):
    high = value.astype(BF16)
    return high, (value - high.astype(F32)).astype(BF16)


def dot_three(left, right, dims=((1,), (0,))):
    lh, ll = halves(left)
    rh, rl = halves(right)
    return dot_any(lh, rh, dims) + (dot_any(lh, rl, dims) + dot_any(ll, rh, dims))


def dot_full(left, right, dims=((1,), (0,))):
    return lax.dot_general(
        left, right, (dims, ((), ())), precision=lax.Precision.HIGHEST, preferred_element_type=F32
    )


def eliminate(matrices):
    size = matrices[0].shape[0]
    groups = size // 8
    lane = lax.broadcasted_iota(jnp.int32, (8, size), 1)
    sub = lax.broadcasted_iota(jnp.int32, (8, size), 0)
    work = [[m[8 * g : 8 * g + 8, :] for g in range(groups)] for m in matrices]
    for k in range(0, size, 2):
        g, r = divmod(k, 8)
        first_lane, second_lane = lane == k, lane == k + 1
        either = first_lane | second_lane
        for rows in work:
            own = rows[g]
            near = jnp.broadcast_to(own[:, k : k + 1], (8, size))
            far = jnp.broadcast_to(own[:, k + 1 : k + 2], (8, size))
            d0 = jnp.broadcast_to(near[r : r + 1, :], (8, size))
            m = jnp.broadcast_to(near[r + 1 : r + 2, :], (8, size))
            e = jnp.broadcast_to(far[r + 1 : r + 2, :], (8, size))
            row0 = jnp.broadcast_to(own[r : r + 1, :], (8, size))
            row1 = jnp.broadcast_to(own[r + 1 : r + 2, :], (8, size))
            i0 = 1.0 / d0
            step = m * i0
            i1 = 1.0 / (e - step * m)
            row0_one = jnp.where(first_lane, 1.0, row0)
            row1_mid = jnp.where(first_lane, 0.0, row1) - step * row0_one
            p0 = jnp.where(second_lane, 0.0, row0_one) * i0
            p1 = jnp.where(second_lane, 1.0, row1_mid) * i1
            for i in range(g, groups):
                if i == g:
                    c0, c1 = near, far
                else:
                    c0 = jnp.broadcast_to(rows[i][:, k : k + 1], (8, size))
                    c1 = jnp.broadcast_to(rows[i][:, k + 1 : k + 2], (8, size))
                c1 = c1 - c0 * step
                new = jnp.where(either, 0.0, rows[i]) - c0 * p0 - c1 * p1
                if i == g:
                    new = jnp.where(sub <= r, own, jnp.where(sub == r + 1, row1_mid, new))
                rows[i] = new
    results = []
    for rows in work:
        pieces = []
        for g in range(groups):
            row = sub + 8 * g
            pivot = jnp.sum(jnp.where(lane == row, rows[g], 0.0), axis=1, keepdims=True)
            unit = jnp.where(lane < row, rows[g], jnp.where(lane == row, 1.0, 0.0))
            pieces.append(unit * lax.rsqrt(pivot))
        results.append(jnp.concatenate(pieces, axis=0))
    return results


def lower_half(value, row, col):
    return jnp.where(row > col, value, jnp.where(row == col, 0.5 * value, 0.0))


def transforms_kernel(
    rho_ref, picked_ref, weight_ref, partial_ref, own_ref, high_ref, low_ref, x_ref, first_inv, second_inv, mid_ref
):
    blocks, windows, slots, members = picked_ref.shape
    half = members // 2
    slot_eye = (
        lax.broadcasted_iota(jnp.int32, (slots, slots), 0)
        == lax.broadcasted_iota(jnp.int32, (slots, slots), 1)
    )
    row = lax.broadcasted_iota(jnp.int32, (members, members), 0)
    col = lax.broadcasted_iota(jnp.int32, (members, members), 1)
    eye = row == col
    nn = ((1,), (0,))
    tn = ((0,), (0,))
    nt = ((1,), (1,))

    for w in range(windows):
        rows = jnp.concatenate([picked_ref[n, w] for n in range(blocks)], axis=0)
        columns = [
            jnp.sum(jnp.where(slot_eye, weight_ref[n, w : w + 1, :], 0.0), axis=1, keepdims=True)
            for n in range(blocks)
        ]
        high, low = halves(rows.astype(F32) * jnp.concatenate(columns, axis=0))
        system = dot_any(high, rows, tn) + dot_any(low, rows, tn) + jnp.where(eye, F32(members - 1.0), 0.0)
        high_ref[w], low_ref[w] = halves(system)
        diagonal = jnp.where(eye, system, 0.0)
        scale_row = lax.rsqrt(jnp.sum(diagonal, axis=0, keepdims=True))
        scale_col = lax.rsqrt(jnp.sum(diagonal, axis=1, keepdims=True))
        corr = system * scale_col * scale_row
        off = jnp.where(eye, 0.0, corr)
        spread = jnp.sum(jnp.sum(off * off, axis=0, keepdims=True), axis=1, keepdims=True)
        beta = 1.0 / (1.0 + SPREAD_GAIN * jnp.sqrt(spread * (1.0 / members)))
        change = lower_half(beta * corr - jnp.where(eye, 1.0, 0.0), row, col)
        narrow = change.astype(BF16)
        second = dot_any(narrow, narrow, nn) + lower_half(dot_any(narrow, narrow, nt), row, col)
        unit = jnp.where(eye, 1.0, 0.0) - change + second
        x_ref[w] = unit * (scale_row * jnp.sqrt(beta))

    def refine(state):
        turn, _ = state
        worst = jnp.zeros((1, 1), F32)
        for w in range(windows):
            x = x_ref[w]
            xh, xl = halves(x)
            ah = high_ref[w]
            left = dot_any(xh, ah, nn) + (dot_any(xh, low_ref[w], nn) + dot_any(xl, ah, nn))
            lh, ll = halves(left)
            near = dot_any(lh, xh, nt) + (dot_any(lh, xl, nt) + dot_any(ll, xh, nt))
            change = lower_half(near - jnp.where(eye, 1.0, 0.0), row, col)
            size = jnp.sum(jnp.sum(change * change, axis=0, keepdims=True), axis=1, keepdims=True)
            worst = jnp.where(size <= worst, worst, size)
            narrow = change.astype(BF16)
            square = lower_half(dot_any(narrow, narrow, nt), row, col).astype(BF16)
            rest = (x - dot_any(narrow, xh, nn)).astype(BF16)
            x_ref[w] = x - dot_any(narrow, rest, nn) + dot_any(square, xh, nn)
        return turn + 1, worst[0, 0]

    def again(state):
        turn, size = state
        return (turn < 8) & (size > SETTLED) & (size < 1.0)

    _, size = lax.while_loop(again, refine, refine((jnp.int32(0), F32(0.5))))

    @pl.when(jnp.logical_not(size <= SETTLED))
    def _():
        direct(high_ref, low_ref, partial_ref, x_ref, first_inv, second_inv, mid_ref)

    for w in range(windows):
        scale = rho_ref[w] * jnp.sqrt(F32(members - 1.0))
        partial_ref[w] = scale * x_ref[w]

    for turn in range(windows - 1):
        w = windows - 2 - turn
        partial_ref[w] = dot_three(partial_ref[w + 1], partial_ref[w])

    own_ref[0] = partial_ref[0, :half, :half].astype(BF16)
    own_ref[1] = partial_ref[0, half:, :half].astype(BF16)
    own_ref[2] = partial_ref[0, half:, half:].astype(BF16)


def direct(high_ref, low_ref, gram, x_ref, first_inv, second_inv, mid_ref):
    windows, members, _ = x_ref.shape
    half = members // 2
    nt = ((1,), (1,))

    for w in range(windows):
        gram[w] = high_ref[w].astype(F32) + low_ref[w].astype(F32)

    for w, value in enumerate(eliminate([gram[w, :half, :half] for w in range(windows)])):
        first_inv[w] = value

    @pl.loop(0, windows)
    def _(w):
        lower = dot_full(gram[w, half:, :half], first_inv[w], nt)
        gram[w, half:, half:] -= dot_full(lower, lower, nt)
        mid_ref[w] = dot_full(lower, first_inv[w])

    for w, value in enumerate(eliminate([gram[w, half:, half:] for w in range(windows)])):
        second_inv[w] = value

    @pl.loop(0, windows)
    def _(w):
        x_ref[w, :half, :half] = first_inv[w]
        x_ref[w, :half, half:] = jnp.zeros((half, half), F32)
        x_ref[w, half:, :half] = -dot_full(second_inv[w], mid_ref[w])
        x_ref[w, half:, half:] = second_inv[w]


def fold_kernel(position_ref, products_ref, partial_ref, out_ref, whole, later):
    count = products_ref.shape[0]
    windows, members, _ = partial_ref.shape
    half = members // 2
    position = position_ref[0]
    whole[...] = jnp.zeros_like(whole)
    later[...] = (
        lax.broadcasted_iota(jnp.int32, (members, members), 0)
        == lax.broadcasted_iota(jnp.int32, (members, members), 1)
    ).astype(F32)

    @pl.loop(0, count - 1 - position)
    def _(turn):
        source = count - 1 - turn
        whole[:half, :half] = products_ref[source, 0]
        whole[half:, :half] = products_ref[source, 1]
        whole[half:, half:] = products_ref[source, 2]
        high, low = halves(later[...])
        right = whole[...]
        later[...] = dot_any(high, right, ((1,), (0,))) + dot_any(low, right, ((1,), (0,)))

    @pl.loop(0, windows)
    def _(w):
        out_ref[w] = dot_three(later[...], partial_ref[w]).astype(BF16)


def exchange_kernel(axis, count, one_way, items, *refs):
    ins, outs = refs[:items], refs[items : 2 * items]
    send_sem, recv_sem = refs[2 * items :]
    me = lax.axis_index(axis)
    barrier = pltpu.get_barrier_semaphore()
    for shift in range(1, count):
        pl.semaphore_signal(
            barrier,
            inc=1,
            device_id={axis: lax.rem(me + shift, count)},
            device_id_type=pl.DeviceIdType.MESH,
        )
    pl.semaphore_wait(barrier, count - 1)

    def copy_of(shift, item):
        return pltpu.make_async_remote_copy(
            src_ref=ins[item],
            dst_ref=outs[item].at[me],
            send_sem=send_sem.at[item, shift],
            recv_sem=recv_sem.at[item, shift],
            device_id={axis: lax.rem(me + count - shift, count)},
            device_id_type=pl.DeviceIdType.MESH,
        )

    def when(condition, action):
        if one_way:
            pl.when(condition)(action)
        else:
            action()

    order = [(shift, item) for shift in range(1, count) for item in range(items)]
    for shift, item in order:
        when(me >= shift, lambda: copy_of(shift, item).start())
    if not one_way:
        for item in range(items):
            outs[item][me] = ins[item][...]
    for shift, item in order:
        when(me >= shift, lambda: copy_of(shift, item).wait_send())
        when(me + shift < count, lambda: copy_of(shift, item).wait_recv())


def exchange(axis, one_way, collective_id, *values):
    count = lax.axis_size(axis)
    items = len(values)
    vmem = pl.BlockSpec(memory_space=pltpu.VMEM)
    return pl.pallas_call(
        lambda *refs: exchange_kernel(axis, count, one_way, items, *refs),
        out_shape=tuple(jax.ShapeDtypeStruct((count,) + v.shape, v.dtype) for v in values),
        in_specs=[vmem] * items,
        out_specs=(vmem,) * items,
        scratch_shapes=[
            pltpu.SemaphoreType.DMA((items, count)),
            pltpu.SemaphoreType.DMA((items, count)),
        ],
        compiler_params=pltpu.CompilerParams(
            collective_id=collective_id, has_side_effects=True, vmem_limit_bytes=8 * MIB
        ),
        cost_estimate=pl.CostEstimate(flops=2 * 10**9, bytes_accessed=MIB, transcendentals=0),
        name="exchange_" + axis,
    )(*values)


def apply_kernel(field_ref, weight_ref, out_ref):
    out_ref[0] = dot_any(field_ref[0], weight_ref[0], ((1,), (1,))).astype(out_ref.dtype)


def local(anomalies, obs_cells, obs_counts, obs_precision, inflation):
    windows, _, cell_width, members = anomalies.shape
    half = members // 2
    slots = obs_cells.shape[1]
    first_cell = lax.axis_index("cell") * cell_width
    offsets = obs_cells - first_cell
    picked = jax.vmap(lambda field, where_at: field[0][where_at])(anomalies, offsets)
    live = jnp.arange(slots, dtype=jnp.int32)[None, :] < obs_counts
    weights = jnp.where(live, obs_precision, jnp.float32(0.0))
    gathered, gathered_weights = exchange("cell", False, 0, picked, weights)
    vmem = pl.BlockSpec(memory_space=pltpu.VMEM)
    smem = pl.BlockSpec(memory_space=pltpu.SMEM)
    partial, own = pl.pallas_call(
        transforms_kernel,
        out_shape=(
            jax.ShapeDtypeStruct((windows, members, members), F32),
            jax.ShapeDtypeStruct((3, half, half), BF16),
        ),
        in_specs=[smem, vmem, vmem],
        out_specs=(vmem, vmem),
        scratch_shapes=[pltpu.VMEM((windows, members, members), BF16)] * 2
        + [pltpu.VMEM((windows, members, members), F32)]
        + [pltpu.VMEM((windows, half, half), F32)] * 3,
        compiler_params=pltpu.CompilerParams(vmem_limit_bytes=16 * MIB),
        cost_estimate=pl.CostEstimate(flops=4 * 10**9, bytes_accessed=2 * MIB, transcendentals=0),
        name="transforms",
    )(inflation, gathered, gathered_weights)
    (products,) = exchange("tm", True, 1, own)
    weight_mats = pl.pallas_call(
        fold_kernel,
        out_shape=jax.ShapeDtypeStruct((windows, members, members), BF16),
        in_specs=[smem, vmem, vmem],
        out_specs=vmem,
        scratch_shapes=[pltpu.VMEM((members, members), BF16), pltpu.VMEM((members, members), F32)],
        compiler_params=pltpu.CompilerParams(vmem_limit_bytes=8 * MIB),
        cost_estimate=pl.CostEstimate(flops=10**9, bytes_accessed=MIB, transcendentals=0),
        name="fold",
    )(lax.axis_index("tm").astype(jnp.int32)[None], products, partial)
    flat = anomalies.reshape(windows, 2 * cell_width, members)
    tile = min(2048, 2 * cell_width)
    result = pl.pallas_call(
        apply_kernel,
        out_shape=jax.ShapeDtypeStruct(flat.shape, BF16),
        grid=(windows, 2 * cell_width // tile),
        in_specs=[
            pl.BlockSpec((1, tile, members), lambda w, c: (w, c, 0)),
            pl.BlockSpec((1, members, members), lambda w, c: (w, 0, 0)),
        ],
        out_specs=pl.BlockSpec((1, tile, members), lambda w, c: (w, c, 0)),
        compiler_params=pltpu.CompilerParams(vmem_limit_bytes=16 * MIB),
        name="apply",
    )(flat, weight_mats)
    return result.reshape(anomalies.shape)


def solution(mesh):
    placed = (
        P("tm", None, "cell", None),
        P("tm", "cell"),
        P("tm", "cell"),
        P("tm", "cell"),
        P("tm"),
    )
    return jax.shard_map(
        local, mesh=mesh, in_specs=placed, out_specs=P("tm", None, "cell", None), check_vma=False
    )
```

```python
import jax
import jax.numpy as jnp
from jax import lax
from jax.experimental import pallas as pl
from jax.experimental.pallas import tpu as pltpu
from jax.sharding import PartitionSpec as P

F32 = jnp.float32
BF16 = jnp.bfloat16
SPREAD_GAIN = 1.4
SETTLED = 4e-4
MIB = 1 << 20


def dot_any(left, right, dims):
    return lax.dot_general(left, right, (dims, ((), ())), preferred_element_type=F32)


def halves(value):
    high = value.astype(BF16)
    return high, (value - high.astype(F32)).astype(BF16)


def dot_three(left, right, dims=((1,), (0,))):
    lh, ll = halves(left)
    rh, rl = halves(right)
    return dot_any(lh, rh, dims) + (dot_any(lh, rl, dims) + dot_any(ll, rh, dims))


def dot_full(left, right, dims=((1,), (0,))):
    return lax.dot_general(
        left, right, (dims, ((), ())), precision=lax.Precision.HIGHEST, preferred_element_type=F32
    )


def eliminate(matrices):
    size = matrices[0].shape[0]
    groups = size // 8
    lane = lax.broadcasted_iota(jnp.int32, (8, size), 1)
    sub = lax.broadcasted_iota(jnp.int32, (8, size), 0)
    work = [[m[8 * g : 8 * g + 8, :] for g in range(groups)] for m in matrices]
    for k in range(0, size, 2):
        g, r = divmod(k, 8)
        first_lane, second_lane = lane == k, lane == k + 1
        either = first_lane | second_lane
        for rows in work:
            own = rows[g]
            near = jnp.broadcast_to(own[:, k : k + 1], (8, size))
            far = jnp.broadcast_to(own[:, k + 1 : k + 2], (8, size))
            d0 = jnp.broadcast_to(near[r : r + 1, :], (8, size))
            m = jnp.broadcast_to(near[r + 1 : r + 2, :], (8, size))
            e = jnp.broadcast_to(far[r + 1 : r + 2, :], (8, size))
            row0 = jnp.broadcast_to(own[r : r + 1, :], (8, size))
            row1 = jnp.broadcast_to(own[r + 1 : r + 2, :], (8, size))
            i0 = 1.0 / d0
            step = m * i0
            i1 = 1.0 / (e - step * m)
            row0_one = jnp.where(first_lane, 1.0, row0)
            row1_mid = jnp.where(first_lane, 0.0, row1) - step * row0_one
            p0 = jnp.where(second_lane, 0.0, row0_one) * i0
            p1 = jnp.where(second_lane, 1.0, row1_mid) * i1
            for i in range(g, groups):
                if i == g:
                    c0, c1 = near, far
                else:
                    c0 = jnp.broadcast_to(rows[i][:, k : k + 1], (8, size))
                    c1 = jnp.broadcast_to(rows[i][:, k + 1 : k + 2], (8, size))
                c1 = c1 - c0 * step
                new = jnp.where(either, 0.0, rows[i]) - c0 * p0 - c1 * p1
                if i == g:
                    new = jnp.where(sub <= r, own, jnp.where(sub == r + 1, row1_mid, new))
                rows[i] = new
    results = []
    for rows in work:
        pieces = []
        for g in range(groups):
            row = sub + 8 * g
            pivot = jnp.sum(jnp.where(lane == row, rows[g], 0.0), axis=1, keepdims=True)
            unit = jnp.where(lane < row, rows[g], jnp.where(lane == row, 1.0, 0.0))
            pieces.append(unit * lax.rsqrt(pivot))
        results.append(jnp.concatenate(pieces, axis=0))
    return results


def lower_half(value, row, col):
    return jnp.where(row > col, value, jnp.where(row == col, 0.5 * value, 0.0))


def transforms_kernel(
    rho_ref, picked_ref, weight_ref, partial_ref, own_ref, high_ref, low_ref, x_ref, first_inv, second_inv, mid_ref
):
    blocks, windows, slots, members = picked_ref.shape
    half = members // 2
    slot_eye = (
        lax.broadcasted_iota(jnp.int32, (slots, slots), 0)
        == lax.broadcasted_iota(jnp.int32, (slots, slots), 1)
    )
    row = lax.broadcasted_iota(jnp.int32, (members, members), 0)
    col = lax.broadcasted_iota(jnp.int32, (members, members), 1)
    eye = row == col
    nn = ((1,), (0,))
    tn = ((0,), (0,))
    nt = ((1,), (1,))

    for w in range(windows):
        rows = jnp.concatenate([picked_ref[n, w] for n in range(blocks)], axis=0)
        columns = [
            jnp.sum(jnp.where(slot_eye, weight_ref[n, w : w + 1, :], 0.0), axis=1, keepdims=True)
            for n in range(blocks)
        ]
        high, low = halves(rows.astype(F32) * jnp.concatenate(columns, axis=0))
        system = dot_any(high, rows, tn) + dot_any(low, rows, tn) + jnp.where(eye, F32(members - 1.0), 0.0)
        high_ref[w], low_ref[w] = halves(system)
        diagonal = jnp.where(eye, system, 0.0)
        scale_row = lax.rsqrt(jnp.sum(diagonal, axis=0, keepdims=True))
        scale_col = lax.rsqrt(jnp.sum(diagonal, axis=1, keepdims=True))
        corr = system * scale_col * scale_row
        off = jnp.where(eye, 0.0, corr)
        spread = jnp.sum(jnp.sum(off * off, axis=0, keepdims=True), axis=1, keepdims=True)
        beta = 1.0 / (1.0 + SPREAD_GAIN * jnp.sqrt(spread * (1.0 / members)))
        change = lower_half(beta * corr - jnp.where(eye, 1.0, 0.0), row, col)
        narrow = change.astype(BF16)
        second = dot_any(narrow, narrow, nn) + lower_half(dot_any(narrow, narrow, nt), row, col)
        unit = jnp.where(eye, 1.0, 0.0) - change + second
        x_ref[w] = unit * (scale_row * jnp.sqrt(beta))

    def refine(state):
        turn, _ = state
        worst = jnp.zeros((1, 1), F32)
        for w in range(windows):
            x = x_ref[w]
            xh, xl = halves(x)
            ah = high_ref[w]
            left = dot_any(xh, ah, nn) + (dot_any(xh, low_ref[w], nn) + dot_any(xl, ah, nn))
            lh, ll = halves(left)
            near = dot_any(lh, xh, nt) + (dot_any(lh, xl, nt) + dot_any(ll, xh, nt))
            change = lower_half(near - jnp.where(eye, 1.0, 0.0), row, col)
            size = jnp.sum(jnp.sum(change * change, axis=0, keepdims=True), axis=1, keepdims=True)
            worst = jnp.where(size <= worst, worst, size)
            narrow = change.astype(BF16)
            square = lower_half(dot_any(narrow, narrow, nt), row, col).astype(BF16)
            rest = (x - dot_any(narrow, xh, nn)).astype(BF16)
            x_ref[w] = x - dot_any(narrow, rest, nn) + dot_any(square, xh, nn)
        return turn + 1, worst[0, 0]

    def again(state):
        turn, size = state
        return (turn < 8) & (size > SETTLED) & (size < 1.0)

    _, size = lax.while_loop(again, refine, refine((jnp.int32(0), F32(0.5))))

    @pl.when(jnp.logical_not(size <= SETTLED))
    def _():
        direct(high_ref, low_ref, partial_ref, x_ref, first_inv, second_inv, mid_ref)

    for w in range(windows):
        scale = rho_ref[w] * jnp.sqrt(F32(members - 1.0))
        partial_ref[w] = scale * x_ref[w]

    for turn in range(windows - 1):
        w = windows - 2 - turn
        partial_ref[w] = dot_three(partial_ref[w + 1], partial_ref[w])

    own_ref[0] = partial_ref[0, :half, :half].astype(BF16)
    own_ref[1] = partial_ref[0, half:, :half].astype(BF16)
    own_ref[2] = partial_ref[0, half:, half:].astype(BF16)


def direct(high_ref, low_ref, gram, x_ref, first_inv, second_inv, mid_ref):
    windows, members, _ = x_ref.shape
    half = members // 2
    nt = ((1,), (1,))

    for w in range(windows):
        gram[w] = high_ref[w].astype(F32) + low_ref[w].astype(F32)

    for w, value in enumerate(eliminate([gram[w, :half, :half] for w in range(windows)])):
        first_inv[w] = value

    @pl.loop(0, windows)
    def _(w):
        lower = dot_full(gram[w, half:, :half], first_inv[w], nt)
        gram[w, half:, half:] -= dot_full(lower, lower, nt)
        mid_ref[w] = dot_full(lower, first_inv[w])

    for w, value in enumerate(eliminate([gram[w, half:, half:] for w in range(windows)])):
        second_inv[w] = value

    @pl.loop(0, windows)
    def _(w):
        x_ref[w, :half, :half] = first_inv[w]
        x_ref[w, :half, half:] = jnp.zeros((half, half), F32)
        x_ref[w, half:, :half] = -dot_full(second_inv[w], mid_ref[w])
        x_ref[w, half:, half:] = second_inv[w]


def exchange_kernel(axis, count, one_way, items, *refs):
    ins, outs = refs[:items], refs[items : 2 * items]
    send_sem, recv_sem = refs[2 * items :]
    me = lax.axis_index(axis)
    barrier = pltpu.get_barrier_semaphore()
    for shift in range(1, count):
        pl.semaphore_signal(
            barrier,
            inc=1,
            device_id={axis: lax.rem(me + shift, count)},
            device_id_type=pl.DeviceIdType.MESH,
        )
    pl.semaphore_wait(barrier, count - 1)

    def copy_of(shift, item):
        return pltpu.make_async_remote_copy(
            src_ref=ins[item],
            dst_ref=outs[item].at[me],
            send_sem=send_sem.at[item, shift],
            recv_sem=recv_sem.at[item, shift],
            device_id={axis: lax.rem(me + count - shift, count)},
            device_id_type=pl.DeviceIdType.MESH,
        )

    def when(condition, action):
        if one_way:
            pl.when(condition)(action)
        else:
            action()

    order = [(shift, item) for shift in range(1, count) for item in range(items)]
    for shift, item in order:
        when(me >= shift, lambda: copy_of(shift, item).start())
    if not one_way:
        for item in range(items):
            outs[item][me] = ins[item][...]
    for shift, item in order:
        when(me >= shift, lambda: copy_of(shift, item).wait_send())
        when(me + shift < count, lambda: copy_of(shift, item).wait_recv())


def exchange(axis, one_way, collective_id, *values):
    count = lax.axis_size(axis)
    items = len(values)
    vmem = pl.BlockSpec(memory_space=pltpu.VMEM)
    return pl.pallas_call(
        lambda *refs: exchange_kernel(axis, count, one_way, items, *refs),
        out_shape=tuple(jax.ShapeDtypeStruct((count,) + v.shape, v.dtype) for v in values),
        in_specs=[vmem] * items,
        out_specs=(vmem,) * items,
        scratch_shapes=[
            pltpu.SemaphoreType.DMA((items, count)),
            pltpu.SemaphoreType.DMA((items, count)),
        ],
        compiler_params=pltpu.CompilerParams(
            collective_id=collective_id, has_side_effects=True, vmem_limit_bytes=8 * MIB
        ),
        cost_estimate=pl.CostEstimate(flops=2 * 10**9, bytes_accessed=MIB, transcendentals=0),
        name="exchange_" + axis,
    )(*values)


def observe_kernel(axis, count, chunk, field_ref, cells_hbm, counts_hbm, precision_hbm,
    rows_ref, weights_ref, dens, cells_ref, counts_ref, precision_ref, small_sem, load_sem, send_sem, recv_sem):
    windows, slots = cells_ref.shape
    depth = dens.shape[1]
    pieces = depth // chunk
    me = lax.axis_index(axis)

    def load_of(w, piece):
        span = pl.ds(piece * chunk, chunk)
        return pltpu.make_async_copy(
            field_ref.at[w, 0, span, :], dens.at[w, span, :], load_sem.at[w, piece]
        )

    small = [
        pltpu.make_async_copy(source, target, small_sem.at[i])
        for i, (source, target) in enumerate(
            ((cells_hbm, cells_ref), (counts_hbm, counts_ref), (precision_hbm, precision_ref))
        )
    ]
    for copy in small:
        copy.start()
    for w in range(windows):
        for piece in range(pieces):
            load_of(w, piece).start()
    barrier = pltpu.get_barrier_semaphore()
    for shift in range(1, count):
        pl.semaphore_signal(
            barrier,
            inc=1,
            device_id={axis: lax.rem(me + shift, count)},
            device_id_type=pl.DeviceIdType.MESH,
        )

    def copy_of(shift, item, source, target):
        return pltpu.make_async_remote_copy(
            src_ref=source,
            dst_ref=target,
            send_sem=send_sem.at[item, shift],
            recv_sem=recv_sem.at[item, shift],
            device_id={axis: lax.rem(me + count - shift, count)},
            device_id_type=pl.DeviceIdType.MESH,
        )

    def rows_copy(shift, w):
        return copy_of(shift, w, rows_ref.at[me, w], rows_ref.at[me, w])

    def weights_copy(shift):
        return copy_of(shift, windows, weights_ref.at[me], weights_ref.at[me])

    for copy in small:
        copy.wait()
    slot = lax.broadcasted_iota(jnp.int32, (windows, slots), 1)
    window = lax.broadcasted_iota(jnp.int32, (windows, slots), 0)
    counts = jnp.zeros((windows, slots), jnp.int32)
    for w in range(windows):
        counts = jnp.where(window == w, counts_ref[w], counts)
    weights_ref[me] = jnp.where(slot < counts, precision_ref[...], 0.0)
    slot_eye = (
        lax.broadcasted_iota(jnp.int32, (slots, slots), 0)
        == lax.broadcasted_iota(jnp.int32, (slots, slots), 1)
    )
    place = lax.broadcasted_iota(jnp.int32, (slots, chunk), 1)
    offsets = (cells_ref[...] - me * depth).astype(F32)
    columns = [
        jnp.sum(jnp.where(slot_eye, offsets[w : w + 1, :], 0.0), axis=1, keepdims=True).astype(
            jnp.int32
        )
        for w in range(windows)
    ]
    for w in range(windows):
        total = jnp.zeros((slots, dens.shape[2]), F32)
        for piece in range(pieces):
            hit = jnp.where(place + piece * chunk == columns[w], 1.0, 0.0).astype(BF16)
            load_of(w, piece).wait()
            total += dot_any(hit, dens[w, pl.ds(piece * chunk, chunk), :], ((1,), (0,)))
        rows_ref[me, w] = total.astype(BF16)
        if w == 0:
            pl.semaphore_wait(barrier, count - 1)
            for shift in range(1, count):
                weights_copy(shift).start()
        for shift in range(1, count):
            rows_copy(shift, w).start()
    for shift in range(1, count):
        weights_copy(shift).wait()
        for w in range(windows):
            rows_copy(shift, w).wait()


def apply_kernel(position_ref, field_ref, products_ref, partial_ref, out_ref, whole, later, stage, sems):
    count = products_ref.shape[0]
    windows, height, members = field_ref.shape
    half = members // 2
    tile = stage.shape[2]
    tiles = height // tile
    nn = ((1,), (0,))
    whole[...] = jnp.zeros_like(whole)
    later[...] = (
        lax.broadcasted_iota(jnp.int32, (members, members), 0)
        == lax.broadcasted_iota(jnp.int32, (members, members), 1)
    ).astype(F32)

    @pl.loop(0, count - 1 - position_ref[0])
    def _(turn):
        source = count - 1 - turn
        whole[:half, :half] = products_ref[source, 0]
        whole[half:, :half] = products_ref[source, 1]
        whole[half:, half:] = products_ref[source, 2]
        high, low = halves(later[...])
        right = whole[...]
        later[...] = dot_any(high, right, nn) + dot_any(low, right, nn)

    def out_of(w, t):
        return pltpu.make_async_copy(
            stage.at[w, t], out_ref.at[w, pl.ds(t * tile, tile), :], sems.at[w, t]
        )

    for w in range(windows):
        weight = dot_three(later[...], partial_ref[w]).astype(BF16)
        for t in range(tiles):
            stage[w, t] = dot_any(
                field_ref[w, pl.ds(t * tile, tile), :], weight, ((1,), (1,))
            ).astype(BF16)
            out_of(w, t).start()
    for w in range(windows):
        for t in range(tiles):
            out_of(w, t).wait()


def local(anomalies, obs_cells, obs_counts, obs_precision, inflation):
    windows, fields, cell_width, members = anomalies.shape
    half = members // 2
    slots = obs_cells.shape[1]
    count = lax.axis_size("cell")
    chunk = min(1024, cell_width)
    vmem = pl.BlockSpec(memory_space=pltpu.VMEM)
    smem = pl.BlockSpec(memory_space=pltpu.SMEM)
    hbm = pl.BlockSpec(memory_space=pltpu.HBM)
    gathered, gathered_weights = pl.pallas_call(
        lambda *refs: observe_kernel("cell", count, chunk, *refs),
        out_shape=(
            jax.ShapeDtypeStruct((count, windows, slots, members), BF16),
            jax.ShapeDtypeStruct((count, windows, slots), F32),
        ),
        in_specs=[hbm] * 4,
        out_specs=(vmem, vmem),
        scratch_shapes=[
            pltpu.VMEM((windows, cell_width, members), BF16),
            pltpu.VMEM((windows, slots), jnp.int32),
            pltpu.SMEM((windows,), jnp.int32),
            pltpu.VMEM((windows, slots), F32),
            pltpu.SemaphoreType.DMA((3,)),
            pltpu.SemaphoreType.DMA((windows, cell_width // chunk)),
            pltpu.SemaphoreType.DMA((windows + 1, count)),
            pltpu.SemaphoreType.DMA((windows + 1, count)),
        ],
        compiler_params=pltpu.CompilerParams(
            collective_id=0, has_side_effects=True, vmem_limit_bytes=12 * MIB
        ),
        cost_estimate=pl.CostEstimate(flops=2 * 10**9, bytes_accessed=MIB, transcendentals=0),
        name="observe",
    )(
        *(
            pltpu.with_memory_space_constraint(value, pltpu.HBM)
            for value in (anomalies, obs_cells, obs_counts.reshape(windows), obs_precision)
        )
    )
    partial, own = pl.pallas_call(
        transforms_kernel,
        out_shape=(
            jax.ShapeDtypeStruct((windows, members, members), F32),
            jax.ShapeDtypeStruct((3, half, half), BF16),
        ),
        in_specs=[smem, vmem, vmem],
        out_specs=(vmem, vmem),
        scratch_shapes=[pltpu.VMEM((windows, members, members), BF16)] * 2
        + [pltpu.VMEM((windows, members, members), F32)]
        + [pltpu.VMEM((windows, half, half), F32)] * 3,
        compiler_params=pltpu.CompilerParams(vmem_limit_bytes=16 * MIB),
        cost_estimate=pl.CostEstimate(flops=4 * 10**9, bytes_accessed=2 * MIB, transcendentals=0),
        name="transforms",
    )(inflation, gathered, gathered_weights)
    (products,) = exchange("tm", True, 1, own)
    flat = anomalies.reshape(windows, fields * cell_width, members)
    tile = min(512, cell_width)
    result = pl.pallas_call(
        apply_kernel,
        out_shape=jax.ShapeDtypeStruct(flat.shape, BF16),
        in_specs=[smem, vmem, vmem, vmem],
        out_specs=hbm,
        scratch_shapes=[
            pltpu.VMEM((members, members), BF16),
            pltpu.VMEM((members, members), F32),
            pltpu.VMEM((windows, fields * cell_width // tile, tile, members), BF16),
            pltpu.SemaphoreType.DMA((windows, fields * cell_width // tile)),
        ],
        compiler_params=pltpu.CompilerParams(vmem_limit_bytes=16 * MIB),
        name="apply",
    )(lax.axis_index("tm").astype(jnp.int32)[None], flat, products, partial)
    return result.reshape(anomalies.shape)


def solution(mesh):
    placed = (
        P("tm", None, "cell", None),
        P("tm", "cell"),
        P("tm", "cell"),
        P("tm", "cell"),
        P("tm"),
    )
    return jax.shard_map(
        local, mesh=mesh, in_specs=placed, out_specs=P("tm", None, "cell", None), check_vma=False
    )
```

```python
import jax
import jax.numpy as jnp
from jax import lax
from jax.experimental import pallas as pl
from jax.experimental.pallas import tpu as pltpu
from jax.sharding import PartitionSpec as P

F32 = jnp.float32
BF16 = jnp.bfloat16
SPREAD_GAIN = 1.4
SETTLED = 4e-4
MIB = 1 << 20


def dot_any(left, right, dims):
    return lax.dot_general(left, right, (dims, ((), ())), preferred_element_type=F32)


def halves(value):
    high = value.astype(BF16)
    return high, (value - high.astype(F32)).astype(BF16)


def dot_three(left, right, dims=((1,), (0,))):
    lh, ll = halves(left)
    rh, rl = halves(right)
    return dot_any(lh, rh, dims) + (dot_any(lh, rl, dims) + dot_any(ll, rh, dims))


def dot_full(left, right, dims=((1,), (0,))):
    return lax.dot_general(
        left, right, (dims, ((), ())), precision=lax.Precision.HIGHEST, preferred_element_type=F32
    )


def eliminate(matrices):
    size = matrices[0].shape[0]
    groups = size // 8
    lane = lax.broadcasted_iota(jnp.int32, (8, size), 1)
    sub = lax.broadcasted_iota(jnp.int32, (8, size), 0)
    work = [[m[8 * g : 8 * g + 8, :] for g in range(groups)] for m in matrices]
    for k in range(0, size, 2):
        g, r = divmod(k, 8)
        first_lane, second_lane = lane == k, lane == k + 1
        either = first_lane | second_lane
        for rows in work:
            own = rows[g]
            near = jnp.broadcast_to(own[:, k : k + 1], (8, size))
            far = jnp.broadcast_to(own[:, k + 1 : k + 2], (8, size))
            d0 = jnp.broadcast_to(near[r : r + 1, :], (8, size))
            m = jnp.broadcast_to(near[r + 1 : r + 2, :], (8, size))
            e = jnp.broadcast_to(far[r + 1 : r + 2, :], (8, size))
            row0 = jnp.broadcast_to(own[r : r + 1, :], (8, size))
            row1 = jnp.broadcast_to(own[r + 1 : r + 2, :], (8, size))
            i0 = 1.0 / d0
            step = m * i0
            i1 = 1.0 / (e - step * m)
            row0_one = jnp.where(first_lane, 1.0, row0)
            row1_mid = jnp.where(first_lane, 0.0, row1) - step * row0_one
            p0 = jnp.where(second_lane, 0.0, row0_one) * i0
            p1 = jnp.where(second_lane, 1.0, row1_mid) * i1
            for i in range(g, groups):
                if i == g:
                    c0, c1 = near, far
                else:
                    c0 = jnp.broadcast_to(rows[i][:, k : k + 1], (8, size))
                    c1 = jnp.broadcast_to(rows[i][:, k + 1 : k + 2], (8, size))
                c1 = c1 - c0 * step
                new = jnp.where(either, 0.0, rows[i]) - c0 * p0 - c1 * p1
                if i == g:
                    new = jnp.where(sub <= r, own, jnp.where(sub == r + 1, row1_mid, new))
                rows[i] = new
    results = []
    for rows in work:
        pieces = []
        for g in range(groups):
            row = sub + 8 * g
            pivot = jnp.sum(jnp.where(lane == row, rows[g], 0.0), axis=1, keepdims=True)
            unit = jnp.where(lane < row, rows[g], jnp.where(lane == row, 1.0, 0.0))
            pieces.append(unit * lax.rsqrt(pivot))
        results.append(jnp.concatenate(pieces, axis=0))
    return results


def lower_half(value, row, col):
    return jnp.where(row > col, value, jnp.where(row == col, 0.5 * value, 0.0))


def transforms_kernel(
    rho_ref, picked_ref, weight_ref, partial_ref, own_ref, high_ref, low_ref, x_ref, first_inv, second_inv, mid_ref
):
    blocks, windows, slots, members = picked_ref.shape
    slot_eye = (
        lax.broadcasted_iota(jnp.int32, (slots, slots), 0)
        == lax.broadcasted_iota(jnp.int32, (slots, slots), 1)
    )
    row = lax.broadcasted_iota(jnp.int32, (members, members), 0)
    col = lax.broadcasted_iota(jnp.int32, (members, members), 1)
    eye = row == col
    nn = ((1,), (0,))
    tn = ((0,), (0,))
    nt = ((1,), (1,))

    for w in range(windows):
        rows = jnp.concatenate([picked_ref[n, w] for n in range(blocks)], axis=0)
        columns = [
            jnp.sum(jnp.where(slot_eye, weight_ref[n, w : w + 1, :], 0.0), axis=1, keepdims=True)
            for n in range(blocks)
        ]
        high, low = halves(rows.astype(F32) * jnp.concatenate(columns, axis=0))
        system = dot_any(high, rows, tn) + dot_any(low, rows, tn) + jnp.where(eye, F32(members - 1.0), 0.0)
        high_ref[w], low_ref[w] = halves(system)
        diagonal = jnp.where(eye, system, 0.0)
        scale_row = lax.rsqrt(jnp.sum(diagonal, axis=0, keepdims=True))
        scale_col = lax.rsqrt(jnp.sum(diagonal, axis=1, keepdims=True))
        corr = system * scale_col * scale_row
        off = jnp.where(eye, 0.0, corr)
        spread = jnp.sum(jnp.sum(off * off, axis=0, keepdims=True), axis=1, keepdims=True)
        beta = 1.0 / (1.0 + SPREAD_GAIN * jnp.sqrt(spread * (1.0 / members)))
        change = lower_half(beta * corr - jnp.where(eye, 1.0, 0.0), row, col)
        narrow = change.astype(BF16)
        second = dot_any(narrow, narrow, nn) + lower_half(dot_any(narrow, narrow, nt), row, col)
        unit = jnp.where(eye, 1.0, 0.0) - change + second
        x_ref[w] = unit * (scale_row * jnp.sqrt(beta))

    def refine(state):
        turn, _ = state
        worst = jnp.zeros((1, 1), F32)
        for w in range(windows):
            x = x_ref[w]
            xh, xl = halves(x)
            ah = high_ref[w]
            left = dot_any(xh, ah, nn) + (dot_any(xh, low_ref[w], nn) + dot_any(xl, ah, nn))
            lh, ll = halves(left)
            near = dot_any(lh, xh, nt) + (dot_any(lh, xl, nt) + dot_any(ll, xh, nt))
            change = lower_half(near - jnp.where(eye, 1.0, 0.0), row, col)
            size = jnp.sum(jnp.sum(change * change, axis=0, keepdims=True), axis=1, keepdims=True)
            worst = jnp.where(size <= worst, worst, size)
            narrow = change.astype(BF16)
            square = lower_half(dot_any(narrow, narrow, nt), row, col).astype(BF16)
            rest = (x - dot_any(narrow, xh, nn)).astype(BF16)
            x_ref[w] = x - dot_any(narrow, rest, nn) + dot_any(square, xh, nn)
        return turn + 1, worst[0, 0]

    def again(state):
        turn, size = state
        return (turn < 8) & (size > SETTLED) & (size < 1.0)

    _, size = lax.while_loop(again, refine, refine((jnp.int32(0), F32(0.5))))

    @pl.when(jnp.logical_not(size <= SETTLED))
    def _():
        direct(high_ref, low_ref, partial_ref, x_ref, first_inv, second_inv, mid_ref)

    for w in range(windows):
        scale = rho_ref[w] * jnp.sqrt(F32(members - 1.0))
        partial_ref[w] = scale * x_ref[w]

    for turn in range(windows - 1):
        w = windows - 2 - turn
        partial_ref[w] = dot_three(partial_ref[w + 1], partial_ref[w])

    own_ref[...] = partial_ref[0].astype(BF16)


def direct(high_ref, low_ref, gram, x_ref, first_inv, second_inv, mid_ref):
    windows, members, _ = x_ref.shape
    half = members // 2
    nt = ((1,), (1,))

    for w in range(windows):
        gram[w] = high_ref[w].astype(F32) + low_ref[w].astype(F32)

    for w, value in enumerate(eliminate([gram[w, :half, :half] for w in range(windows)])):
        first_inv[w] = value

    @pl.loop(0, windows)
    def _(w):
        lower = dot_full(gram[w, half:, :half], first_inv[w], nt)
        gram[w, half:, half:] -= dot_full(lower, lower, nt)
        mid_ref[w] = dot_full(lower, first_inv[w])

    for w, value in enumerate(eliminate([gram[w, half:, half:] for w in range(windows)])):
        second_inv[w] = value

    @pl.loop(0, windows)
    def _(w):
        x_ref[w, :half, :half] = first_inv[w]
        x_ref[w, :half, half:] = jnp.zeros((half, half), F32)
        x_ref[w, half:, :half] = -dot_full(second_inv[w], mid_ref[w])
        x_ref[w, half:, half:] = second_inv[w]


def suffix_kernel(
    axis, count, own_ref, later_ref, other, mine, wholes, pair_sem, send_sem, recv_sem, pass_send, pass_recv
):
    members = own_ref.shape[0]
    half = members // 2
    chips = count // 2
    me = lax.axis_index(axis)
    chip, core = lax.div(me, 2), lax.rem(me, 2)
    partner = me + 1 - 2 * core
    nn = ((1,), (0,))
    left, right = pl.ds(0, half), pl.ds(half, half)
    split = half + half // 2
    pieces = (
        (pl.ds(0, split), left),
        (pl.ds(split, members - split), left),
        (right, right),
    )
    owned = ((0,), (1, 2))

    for shift in range(1, chips):
        wholes[shift, :half, half:] = jnp.zeros((half, half), BF16)
    barrier = pltpu.get_barrier_semaphore()

    def greet(device):
        pl.semaphore_signal(
            barrier, inc=1, device_id={axis: device}, device_id_type=pl.DeviceIdType.MESH
        )

    greet(partner)
    for shift in range(1, chips):
        greet(lax.rem(me + 2 * shift, count))
    pl.semaphore_wait(barrier, chips)

    def copy_to(device, source, target, send, recv):
        return pltpu.make_async_remote_copy(
            src_ref=source,
            dst_ref=target,
            send_sem=send,
            recv_sem=recv,
            device_id={axis: device},
            device_id_type=pl.DeviceIdType.MESH,
        )

    def down(shift, p):
        rows, cols = pieces[p]
        return copy_to(
            lax.rem(me + count - 2 * shift, count),
            mine.at[rows, cols],
            wholes.at[shift, rows, cols],
            send_sem.at[shift, p],
            recv_sem.at[shift, p],
        )

    def across(shift, p):
        rows, cols = pieces[p]
        place = wholes.at[shift, rows, cols]
        return copy_to(partner, place, place, pass_send.at[shift, p], pass_recv.at[shift, p])

    pair = copy_to(partner, own_ref, other, pair_sem.at[0], pair_sem.at[1])
    pair.start()
    pair.wait()
    first = core == 0
    low_rows, high_rows = own_ref[...], other[...]
    later_left = jnp.where(first, high_rows, low_rows)
    later_right = jnp.where(first, low_rows, high_rows)
    mine[...] = dot_any(later_left, later_right, nn).astype(BF16)

    for k in range(2):
        for shift in range(chips - 1, 0, -1):

            @pl.when((core == k) & (chip >= shift))
            def _():
                for p in owned[k]:
                    down(shift, p).start()

    for k in range(2):
        for shift in range(1, chips):

            @pl.when((core == k) & (chip + shift < chips))
            def _():
                for p in owned[k]:
                    down(shift, p).wait_recv()
                    across(shift, p).start()

    row = lax.broadcasted_iota(jnp.int32, (members, members), 0)
    col = lax.broadcasted_iota(jnp.int32, (members, members), 1)
    later_ref[...] = jnp.where(first, high_rows.astype(F32), jnp.where(row == col, 1.0, 0.0))
    for shift in range(1, chips):

        @pl.when(chip + shift < chips)
        def _():
            for k in range(2):

                @pl.when(core == k)
                def _():
                    for p in owned[1 - k]:
                        across(shift, p).wait_recv()

            high, low = halves(later_ref[...])
            whole = wholes[shift]
            later_ref[...] = dot_any(whole, high, nn) + dot_any(whole, low, nn)

    for k in range(2):
        for shift in range(1, chips):

            @pl.when((core == k) & (chip >= shift))
            def _():
                for p in owned[k]:
                    down(shift, p).wait_send()

            @pl.when((core == k) & (chip + shift < chips))
            def _():
                for p in owned[k]:
                    across(shift, p).wait_send()


def observe_kernel(axis, count, chunk, field_ref, cells_hbm, counts_hbm, precision_hbm,
    rows_ref, weights_ref, dens, cells_ref, counts_ref, precision_ref, small_sem, load_sem, send_sem, recv_sem):
    windows, slots = cells_ref.shape
    depth = dens.shape[1]
    pieces = depth // chunk
    me = lax.axis_index(axis)

    def load_of(w, piece):
        span = pl.ds(piece * chunk, chunk)
        return pltpu.make_async_copy(
            field_ref.at[w, 0, span, :], dens.at[w, span, :], load_sem.at[w, piece]
        )

    small = [
        pltpu.make_async_copy(source, target, small_sem.at[i])
        for i, (source, target) in enumerate(
            ((cells_hbm, cells_ref), (counts_hbm, counts_ref), (precision_hbm, precision_ref))
        )
    ]
    for copy in small:
        copy.start()
    for w in range(windows):
        for piece in range(pieces):
            load_of(w, piece).start()
    barrier = pltpu.get_barrier_semaphore()
    for shift in range(1, count):
        pl.semaphore_signal(
            barrier,
            inc=1,
            device_id={axis: lax.rem(me + shift, count)},
            device_id_type=pl.DeviceIdType.MESH,
        )

    def copy_of(shift, item, source, target):
        return pltpu.make_async_remote_copy(
            src_ref=source,
            dst_ref=target,
            send_sem=send_sem.at[item, shift],
            recv_sem=recv_sem.at[item, shift],
            device_id={axis: lax.rem(me + count - shift, count)},
            device_id_type=pl.DeviceIdType.MESH,
        )

    def rows_copy(shift, w):
        return copy_of(shift, w, rows_ref.at[me, w], rows_ref.at[me, w])

    def weights_copy(shift):
        return copy_of(shift, windows, weights_ref.at[me], weights_ref.at[me])

    for copy in small:
        copy.wait()
    slot = lax.broadcasted_iota(jnp.int32, (windows, slots), 1)
    window = lax.broadcasted_iota(jnp.int32, (windows, slots), 0)
    counts = jnp.zeros((windows, slots), jnp.int32)
    for w in range(windows):
        counts = jnp.where(window == w, counts_ref[w], counts)
    weights_ref[me] = jnp.where(slot < counts, precision_ref[...], 0.0)
    slot_eye = (
        lax.broadcasted_iota(jnp.int32, (slots, slots), 0)
        == lax.broadcasted_iota(jnp.int32, (slots, slots), 1)
    )
    place = lax.broadcasted_iota(jnp.int32, (slots, chunk), 1)
    offsets = (cells_ref[...] - me * depth).astype(F32)
    columns = [
        jnp.sum(jnp.where(slot_eye, offsets[w : w + 1, :], 0.0), axis=1, keepdims=True).astype(
            jnp.int32
        )
        for w in range(windows)
    ]
    for w in range(windows):
        total = jnp.zeros((slots, dens.shape[2]), F32)
        for piece in range(pieces):
            hit = jnp.where(place + piece * chunk == columns[w], 1.0, 0.0).astype(BF16)
            load_of(w, piece).wait()
            total += dot_any(hit, dens[w, pl.ds(piece * chunk, chunk), :], ((1,), (0,)))
        rows_ref[me, w] = total.astype(BF16)
        if w == 0:
            pl.semaphore_wait(barrier, count - 1)
            for shift in range(1, count):
                weights_copy(shift).start()
        for shift in range(1, count):
            rows_copy(shift, w).start()
    for shift in range(1, count):
        weights_copy(shift).wait()
        for w in range(windows):
            rows_copy(shift, w).wait()


def apply_kernel(field_ref, later_ref, partial_ref, out_ref, stage, sems):
    windows, height, _ = field_ref.shape
    tile = stage.shape[2]
    tiles = height // tile

    def out_of(w, t):
        return pltpu.make_async_copy(
            stage.at[w, t], out_ref.at[w, pl.ds(t * tile, tile), :], sems.at[w, t]
        )

    for w in range(windows):
        weight = dot_three(later_ref[...], partial_ref[w]).astype(BF16)
        for t in range(tiles):
            stage[w, t] = dot_any(
                field_ref[w, pl.ds(t * tile, tile), :], weight, ((1,), (1,))
            ).astype(BF16)
            out_of(w, t).start()
    for w in range(windows):
        for t in range(tiles):
            out_of(w, t).wait()


def local(anomalies, obs_cells, obs_counts, obs_precision, inflation):
    windows, fields, cell_width, members = anomalies.shape
    half = members // 2
    slots = obs_cells.shape[1]
    count = lax.axis_size("cell")
    chunk = min(1024, cell_width)
    vmem = pl.BlockSpec(memory_space=pltpu.VMEM)
    smem = pl.BlockSpec(memory_space=pltpu.SMEM)
    hbm = pl.BlockSpec(memory_space=pltpu.HBM)
    gathered, gathered_weights = pl.pallas_call(
        lambda *refs: observe_kernel("cell", count, chunk, *refs),
        out_shape=(
            jax.ShapeDtypeStruct((count, windows, slots, members), BF16),
            jax.ShapeDtypeStruct((count, windows, slots), F32),
        ),
        in_specs=[hbm] * 4,
        out_specs=(vmem, vmem),
        scratch_shapes=[
            pltpu.VMEM((windows, cell_width, members), BF16),
            pltpu.VMEM((windows, slots), jnp.int32),
            pltpu.SMEM((windows,), jnp.int32),
            pltpu.VMEM((windows, slots), F32),
            pltpu.SemaphoreType.DMA((3,)),
            pltpu.SemaphoreType.DMA((windows, cell_width // chunk)),
            pltpu.SemaphoreType.DMA((windows + 1, count)),
            pltpu.SemaphoreType.DMA((windows + 1, count)),
        ],
        compiler_params=pltpu.CompilerParams(
            collective_id=0, has_side_effects=True, vmem_limit_bytes=12 * MIB
        ),
        cost_estimate=pl.CostEstimate(flops=2 * 10**9, bytes_accessed=MIB, transcendentals=0),
        name="observe",
    )(
        *(
            pltpu.with_memory_space_constraint(value, pltpu.HBM)
            for value in (anomalies, obs_cells, obs_counts.reshape(windows), obs_precision)
        )
    )
    partial, own = pl.pallas_call(
        transforms_kernel,
        out_shape=(
            jax.ShapeDtypeStruct((windows, members, members), F32),
            jax.ShapeDtypeStruct((members, members), BF16),
        ),
        in_specs=[smem, vmem, vmem],
        out_specs=(vmem, vmem),
        scratch_shapes=[pltpu.VMEM((windows, members, members), BF16)] * 2
        + [pltpu.VMEM((windows, members, members), F32)]
        + [pltpu.VMEM((windows, half, half), F32)] * 3,
        compiler_params=pltpu.CompilerParams(vmem_limit_bytes=16 * MIB),
        cost_estimate=pl.CostEstimate(flops=4 * 10**9, bytes_accessed=2 * MIB, transcendentals=0),
        name="transforms",
    )(inflation, gathered, gathered_weights)
    devices = lax.axis_size("tm")
    hops = pltpu.SemaphoreType.DMA((devices // 2, 3))
    later = pl.pallas_call(
        lambda *refs: suffix_kernel("tm", devices, *refs),
        out_shape=jax.ShapeDtypeStruct((members, members), F32),
        in_specs=[vmem],
        out_specs=vmem,
        scratch_shapes=[
            pltpu.VMEM((members, members), BF16),
            pltpu.VMEM((members, members), BF16),
            pltpu.VMEM((devices // 2, members, members), BF16),
            pltpu.SemaphoreType.DMA((2,)),
        ]
        + [hops] * 4,
        compiler_params=pltpu.CompilerParams(
            collective_id=1, has_side_effects=True, vmem_limit_bytes=8 * MIB
        ),
        cost_estimate=pl.CostEstimate(flops=2 * 10**9, bytes_accessed=MIB, transcendentals=0),
        name="suffix",
    )(own)
    flat = anomalies.reshape(windows, fields * cell_width, members)
    tile = min(512, cell_width)
    result = pl.pallas_call(
        apply_kernel,
        out_shape=jax.ShapeDtypeStruct(flat.shape, BF16),
        in_specs=[vmem, vmem, vmem],
        out_specs=hbm,
        scratch_shapes=[
            pltpu.VMEM((windows, fields * cell_width // tile, tile, members), BF16),
            pltpu.SemaphoreType.DMA((windows, fields * cell_width // tile)),
        ],
        compiler_params=pltpu.CompilerParams(vmem_limit_bytes=16 * MIB),
        name="apply",
    )(flat, later, partial)
    return result.reshape(anomalies.shape)


def solution(mesh):
    placed = (
        P("tm", None, "cell", None),
        P("tm", "cell"),
        P("tm", "cell"),
        P("tm", "cell"),
        P("tm"),
    )
    return jax.shard_map(
        local, mesh=mesh, in_specs=placed, out_specs=P("tm", None, "cell", None), check_vma=False
    )
```

```python
import jax
import jax.numpy as jnp
from jax import lax
from jax.experimental import pallas as pl
from jax.experimental.pallas import tpu as pltpu
from jax.sharding import PartitionSpec as P

F32 = jnp.float32
BF16 = jnp.bfloat16
SPREAD_GAIN = 1.4
SETTLED = 2e-3
MIB = 1 << 20


def dot_any(left, right, dims):
    return lax.dot_general(left, right, (dims, ((), ())), preferred_element_type=F32)


def halves(value):
    high = value.astype(BF16)
    return high, (value - high.astype(F32)).astype(BF16)


def dot_three(left, right, dims=((1,), (0,))):
    lh, ll = halves(left)
    rh, rl = halves(right)
    return dot_any(lh, rh, dims) + (dot_any(lh, rl, dims) + dot_any(ll, rh, dims))


def dot_full(left, right, dims=((1,), (0,))):
    return lax.dot_general(
        left, right, (dims, ((), ())), precision=lax.Precision.HIGHEST, preferred_element_type=F32
    )


def eliminate(matrices):
    size = matrices[0].shape[0]
    groups = size // 8
    lane = lax.broadcasted_iota(jnp.int32, (8, size), 1)
    sub = lax.broadcasted_iota(jnp.int32, (8, size), 0)
    work = [[m[8 * g : 8 * g + 8, :] for g in range(groups)] for m in matrices]
    for k in range(0, size, 2):
        g, r = divmod(k, 8)
        first_lane, second_lane = lane == k, lane == k + 1
        either = first_lane | second_lane
        for rows in work:
            own = rows[g]
            near = jnp.broadcast_to(own[:, k : k + 1], (8, size))
            far = jnp.broadcast_to(own[:, k + 1 : k + 2], (8, size))
            d0 = jnp.broadcast_to(near[r : r + 1, :], (8, size))
            m = jnp.broadcast_to(near[r + 1 : r + 2, :], (8, size))
            e = jnp.broadcast_to(far[r + 1 : r + 2, :], (8, size))
            row0 = jnp.broadcast_to(own[r : r + 1, :], (8, size))
            row1 = jnp.broadcast_to(own[r + 1 : r + 2, :], (8, size))
            i0 = 1.0 / d0
            step = m * i0
            i1 = 1.0 / (e - step * m)
            row0_one = jnp.where(first_lane, 1.0, row0)
            row1_mid = jnp.where(first_lane, 0.0, row1) - step * row0_one
            p0 = jnp.where(second_lane, 0.0, row0_one) * i0
            p1 = jnp.where(second_lane, 1.0, row1_mid) * i1
            for i in range(g, groups):
                if i == g:
                    c0, c1 = near, far
                else:
                    c0 = jnp.broadcast_to(rows[i][:, k : k + 1], (8, size))
                    c1 = jnp.broadcast_to(rows[i][:, k + 1 : k + 2], (8, size))
                c1 = c1 - c0 * step
                new = jnp.where(either, 0.0, rows[i]) - c0 * p0 - c1 * p1
                if i == g:
                    new = jnp.where(sub <= r, own, jnp.where(sub == r + 1, row1_mid, new))
                rows[i] = new
    results = []
    for rows in work:
        pieces = []
        for g in range(groups):
            row = sub + 8 * g
            pivot = jnp.sum(jnp.where(lane == row, rows[g], 0.0), axis=1, keepdims=True)
            unit = jnp.where(lane < row, rows[g], jnp.where(lane == row, 1.0, 0.0))
            pieces.append(unit * lax.rsqrt(pivot))
        results.append(jnp.concatenate(pieces, axis=0))
    return results


def lower_half(value, row, col):
    return jnp.where(row > col, value, jnp.where(row == col, 0.5 * value, 0.0))


def transforms_kernel(
    rho_ref, picked_ref, weight_ref, partial_ref, own_ref, high_ref, low_ref, x_ref, first_inv, second_inv, mid_ref
):
    blocks, windows, slots, members = picked_ref.shape
    slot_eye = (
        lax.broadcasted_iota(jnp.int32, (slots, slots), 0)
        == lax.broadcasted_iota(jnp.int32, (slots, slots), 1)
    )
    row = lax.broadcasted_iota(jnp.int32, (members, members), 0)
    col = lax.broadcasted_iota(jnp.int32, (members, members), 1)
    eye = row == col
    nn = ((1,), (0,))
    tn = ((0,), (0,))
    nt = ((1,), (1,))

    unit = jnp.where(eye, 1.0, 0.0)

    every = range(windows)

    def squares(changes):
        narrow = [change.astype(BF16) for change in changes]
        plain = [dot_any(n, n, nn) for n in narrow]
        crossed = [dot_any(n, n, nt) for n in narrow]
        return [p + lower_half(c, row, col) for p, c in zip(plain, crossed)]

    def correct(narrow_x, changes):
        steps = [(c - s).astype(BF16) for c, s in zip(changes, squares(changes))]
        moves = [dot_any(step, narrow_x[w], nn) for w, step in enumerate(steps)]
        for w in every:
            x_ref[w] -= moves[w]

    rows = [jnp.concatenate([picked_ref[n, w] for n in range(blocks)], axis=0) for w in every]
    columns = [
        jnp.concatenate(
            [
                jnp.sum(
                    jnp.where(slot_eye, weight_ref[n, w : w + 1, :], 0.0), axis=1, keepdims=True
                )
                for n in range(blocks)
            ],
            axis=0,
        )
        for w in every
    ]
    wide = [value.astype(F32) for value in rows]
    scaled = [wide[w] * columns[w] for w in every]
    scale_rows = [
        jnp.sqrt(1.0 / (jnp.sum(scaled[w] * wide[w], axis=0, keepdims=True) + F32(members - 1.0)))
        for w in every
    ]
    near_rows = [(wide[w] * (jnp.sqrt(columns[w]) * scale_rows[w])).astype(BF16) for w in every]
    offs = [jnp.where(eye, 0.0, dot_any(value, value, tn)) for value in near_rows]
    splits = [halves(value) for value in scaled]
    for w in every:
        system = dot_any(rows[w], splits[w][0], tn) + dot_any(rows[w], splits[w][1], tn)
        high_ref[w], low_ref[w] = halves(system + F32(members - 1.0) * unit)
    spreads = [
        jnp.sum(jnp.sum(off * off, axis=0, keepdims=True), axis=1, keepdims=True) for off in offs
    ]
    betas = [1.0 / (1.0 + SPREAD_GAIN * jnp.sqrt(spread * (1.0 / members))) for spread in spreads]
    changes = [
        jnp.where(row > col, beta * off, jnp.where(eye, 0.5 * (beta - 1.0), 0.0))
        for beta, off in zip(betas, offs)
    ]
    scales = [scale_rows[w] * jnp.sqrt(betas[w]) for w in every]

    for w, second in enumerate(squares(changes)):
        x_ref[w] = (unit - changes[w] + second) * scales[w]

    xh = [x_ref[w].astype(BF16) for w in every]
    left = [dot_any(xh[w], high_ref[w], nn).astype(BF16) for w in every]
    correct(xh, [lower_half(dot_any(left[w], xh[w], nt) - unit, row, col) for w in every])

    def refine(state):
        turn, _ = state
        worst = jnp.zeros((1, 1), F32)
        xs = [halves(x_ref[w]) for w in every]
        left = [
            dot_any(xs[w][0], high_ref[w], nn)
            + (dot_any(xs[w][0], low_ref[w], nn) + dot_any(xs[w][1], high_ref[w], nn))
            for w in every
        ]
        ls = [halves(value) for value in left]
        near = [
            dot_any(ls[w][0], xs[w][0], nt)
            + (dot_any(ls[w][0], xs[w][1], nt) + dot_any(ls[w][1], xs[w][0], nt))
            for w in every
        ]
        changes = [lower_half(value - unit, row, col) for value in near]
        for change in changes:
            size = jnp.sum(jnp.sum(change * change, axis=0, keepdims=True), axis=1, keepdims=True)
            worst = jnp.where(size <= worst, worst, size)
        correct([x[0] for x in xs], changes)
        return turn + 1, worst[0, 0]

    def again(state):
        turn, size = state
        return (turn < 8) & (size > SETTLED) & (size < 1.0)

    _, size = lax.while_loop(again, refine, refine((jnp.int32(0), F32(0.5))))

    @pl.when(jnp.logical_not(size <= SETTLED))
    def _():
        direct(high_ref, low_ref, partial_ref, x_ref, first_inv, second_inv, mid_ref)

    for w in range(windows):
        scale = rho_ref[w] * jnp.sqrt(F32(members - 1.0))
        partial_ref[w] = scale * x_ref[w]

    for turn in range(windows - 1):
        w = windows - 2 - turn
        partial_ref[w] = dot_three(partial_ref[w + 1], partial_ref[w])

    own_ref[...] = partial_ref[0].astype(BF16)


def direct(high_ref, low_ref, gram, x_ref, first_inv, second_inv, mid_ref):
    windows, members, _ = x_ref.shape
    half = members // 2
    nt = ((1,), (1,))

    for w in range(windows):
        gram[w] = high_ref[w].astype(F32) + low_ref[w].astype(F32)

    for w, value in enumerate(eliminate([gram[w, :half, :half] for w in range(windows)])):
        first_inv[w] = value

    @pl.loop(0, windows)
    def _(w):
        lower = dot_full(gram[w, half:, :half], first_inv[w], nt)
        gram[w, half:, half:] -= dot_full(lower, lower, nt)
        mid_ref[w] = dot_full(lower, first_inv[w])

    for w, value in enumerate(eliminate([gram[w, half:, half:] for w in range(windows)])):
        second_inv[w] = value

    @pl.loop(0, windows)
    def _(w):
        x_ref[w, :half, :half] = first_inv[w]
        x_ref[w, :half, half:] = jnp.zeros((half, half), F32)
        x_ref[w, half:, :half] = -dot_full(second_inv[w], mid_ref[w])
        x_ref[w, half:, half:] = second_inv[w]


def suffix_kernel(
    axis, count, own_ref, later_ref, other, mine, wholes, pair_sem, send_sem, recv_sem, pass_send, pass_recv
):
    members = own_ref.shape[0]
    half = members // 2
    chips = count // 2
    me = lax.axis_index(axis)
    chip, core = lax.div(me, 2), lax.rem(me, 2)
    partner = me + 1 - 2 * core
    nn = ((1,), (0,))
    left, right = pl.ds(0, half), pl.ds(half, half)
    split = half + half // 2
    pieces = (
        (pl.ds(0, split), left),
        (pl.ds(split, members - split), left),
        (right, right),
    )
    owned = ((0,), (1, 2))

    for shift in range(1, chips):
        wholes[shift, :half, half:] = jnp.zeros((half, half), BF16)
    barrier = pltpu.get_barrier_semaphore()

    def greet(device):
        pl.semaphore_signal(
            barrier, inc=1, device_id={axis: device}, device_id_type=pl.DeviceIdType.MESH
        )

    greet(partner)
    for shift in range(1, chips):
        greet(lax.rem(me + 2 * shift, count))
    pl.semaphore_wait(barrier, chips)

    def copy_to(device, source, target, send, recv):
        return pltpu.make_async_remote_copy(
            src_ref=source,
            dst_ref=target,
            send_sem=send,
            recv_sem=recv,
            device_id={axis: device},
            device_id_type=pl.DeviceIdType.MESH,
        )

    def down(shift, p):
        rows, cols = pieces[p]
        return copy_to(
            lax.rem(me + count - 2 * shift, count),
            mine.at[rows, cols],
            wholes.at[shift, rows, cols],
            send_sem.at[shift, p],
            recv_sem.at[shift, p],
        )

    def across(shift, p):
        rows, cols = pieces[p]
        place = wholes.at[shift, rows, cols]
        return copy_to(partner, place, place, pass_send.at[shift, p], pass_recv.at[shift, p])

    pair = copy_to(partner, own_ref, other, pair_sem.at[0], pair_sem.at[1])
    pair.start()
    pair.wait()
    first = core == 0
    low_rows, high_rows = own_ref[...], other[...]
    later_left = jnp.where(first, high_rows, low_rows)
    later_right = jnp.where(first, low_rows, high_rows)
    mine[...] = dot_any(later_left, later_right, nn).astype(BF16)

    for k in range(2):
        for shift in range(chips - 1, 0, -1):

            @pl.when((core == k) & (chip >= shift))
            def _():
                for p in owned[k]:
                    down(shift, p).start()

    for k in range(2):
        for shift in range(1, chips):

            @pl.when((core == k) & (chip + shift < chips))
            def _():
                for p in owned[k]:
                    down(shift, p).wait_recv()
                    across(shift, p).start()

    row = lax.broadcasted_iota(jnp.int32, (members, members), 0)
    col = lax.broadcasted_iota(jnp.int32, (members, members), 1)
    later_ref[...] = jnp.where(first, high_rows.astype(F32), jnp.where(row == col, 1.0, 0.0))
    for shift in range(1, chips):

        @pl.when(chip + shift < chips)
        def _():
            for k in range(2):

                @pl.when(core == k)
                def _():
                    for p in owned[1 - k]:
                        across(shift, p).wait_recv()

            high, low = halves(later_ref[...])
            whole = wholes[shift]
            later_ref[...] = dot_any(whole, high, nn) + dot_any(whole, low, nn)

    for k in range(2):
        for shift in range(1, chips):

            @pl.when((core == k) & (chip >= shift))
            def _():
                for p in owned[k]:
                    down(shift, p).wait_send()

            @pl.when((core == k) & (chip + shift < chips))
            def _():
                for p in owned[k]:
                    across(shift, p).wait_send()


def observe_kernel(axis, count, chunk, field_ref, cells_hbm, counts_hbm, precision_hbm,
    rows_ref, weights_ref, dens, cells_ref, counts_ref, precision_ref, small_sem, load_sem, send_sem, recv_sem):
    windows, slots = cells_ref.shape
    depth = dens.shape[1]
    pieces = depth // chunk
    me = lax.axis_index(axis)

    def load_of(w, piece):
        span = pl.ds(piece * chunk, chunk)
        return pltpu.make_async_copy(
            field_ref.at[w, 0, span, :], dens.at[w, span, :], load_sem.at[w, piece]
        )

    small = [
        pltpu.make_async_copy(source, target, small_sem.at[i])
        for i, (source, target) in enumerate(
            ((cells_hbm, cells_ref), (counts_hbm, counts_ref), (precision_hbm, precision_ref))
        )
    ]
    for copy in small:
        copy.start()
    for w in range(windows):
        for piece in range(pieces):
            load_of(w, piece).start()
    barrier = pltpu.get_barrier_semaphore()
    for shift in range(1, count):
        pl.semaphore_signal(
            barrier,
            inc=1,
            device_id={axis: lax.rem(me + shift, count)},
            device_id_type=pl.DeviceIdType.MESH,
        )

    def copy_of(shift, item, source, target):
        return pltpu.make_async_remote_copy(
            src_ref=source,
            dst_ref=target,
            send_sem=send_sem.at[item, shift],
            recv_sem=recv_sem.at[item, shift],
            device_id={axis: lax.rem(me + count - shift, count)},
            device_id_type=pl.DeviceIdType.MESH,
        )

    def rows_copy(shift, w):
        return copy_of(shift, w, rows_ref.at[me, w], rows_ref.at[me, w])

    def weights_copy(shift):
        return copy_of(shift, windows, weights_ref.at[me], weights_ref.at[me])

    for copy in small:
        copy.wait()
    slot = lax.broadcasted_iota(jnp.int32, (windows, slots), 1)
    window = lax.broadcasted_iota(jnp.int32, (windows, slots), 0)
    counts = jnp.zeros((windows, slots), jnp.int32)
    for w in range(windows):
        counts = jnp.where(window == w, counts_ref[w], counts)
    weights_ref[me] = jnp.where(slot < counts, precision_ref[...], 0.0)
    slot_eye = (
        lax.broadcasted_iota(jnp.int32, (slots, slots), 0)
        == lax.broadcasted_iota(jnp.int32, (slots, slots), 1)
    )
    place = lax.broadcasted_iota(jnp.int32, (slots, chunk), 1)
    offsets = (cells_ref[...] - me * depth).astype(F32)
    columns = [
        jnp.sum(jnp.where(slot_eye, offsets[w : w + 1, :], 0.0), axis=1, keepdims=True).astype(
            jnp.int32
        )
        for w in range(windows)
    ]
    for w in range(windows):
        total = jnp.zeros((slots, dens.shape[2]), F32)
        for piece in range(pieces):
            hit = jnp.where(place + piece * chunk == columns[w], 1.0, 0.0).astype(BF16)
            load_of(w, piece).wait()
            total += dot_any(hit, dens[w, pl.ds(piece * chunk, chunk), :], ((1,), (0,)))
        rows_ref[me, w] = total.astype(BF16)
        if w == 0:
            pl.semaphore_wait(barrier, count - 1)
            for shift in range(1, count):
                weights_copy(shift).start()
        for shift in range(1, count):
            rows_copy(shift, w).start()
    for shift in range(1, count):
        weights_copy(shift).wait()
        for w in range(windows):
            rows_copy(shift, w).wait()


def apply_kernel(field_ref, later_ref, partial_ref, out_ref, stage, sems):
    windows, height, _ = field_ref.shape
    tile = stage.shape[2]
    tiles = height // tile
    nn = ((1,), (0,))

    def out_of(w, t):
        return pltpu.make_async_copy(
            stage.at[w, t], out_ref.at[w, pl.ds(t * tile, tile), :], sems.at[w, t]
        )

    high, low = halves(later_ref[...])
    parts = [halves(partial_ref[w]) for w in range(windows)]
    weights = [
        (
            dot_any(high, parts[w][0], nn)
            + (dot_any(high, parts[w][1], nn) + dot_any(low, parts[w][0], nn))
        ).astype(BF16)
        for w in range(windows)
    ]
    for w in range(windows):
        for t in range(tiles):
            stage[w, t] = dot_any(
                field_ref[w, pl.ds(t * tile, tile), :], weights[w], ((1,), (1,))
            ).astype(BF16)
            out_of(w, t).start()
    for w in range(windows):
        for t in range(tiles):
            out_of(w, t).wait()


def local(anomalies, obs_cells, obs_counts, obs_precision, inflation):
    windows, fields, cell_width, members = anomalies.shape
    half = members // 2
    slots = obs_cells.shape[1]
    count = lax.axis_size("cell")
    chunk = min(1024, cell_width)
    vmem = pl.BlockSpec(memory_space=pltpu.VMEM)
    smem = pl.BlockSpec(memory_space=pltpu.SMEM)
    hbm = pl.BlockSpec(memory_space=pltpu.HBM)
    gathered, gathered_weights = pl.pallas_call(
        lambda *refs: observe_kernel("cell", count, chunk, *refs),
        out_shape=(
            jax.ShapeDtypeStruct((count, windows, slots, members), BF16),
            jax.ShapeDtypeStruct((count, windows, slots), F32),
        ),
        in_specs=[hbm] * 4,
        out_specs=(vmem, vmem),
        scratch_shapes=[
            pltpu.VMEM((windows, cell_width, members), BF16),
            pltpu.VMEM((windows, slots), jnp.int32),
            pltpu.SMEM((windows,), jnp.int32),
            pltpu.VMEM((windows, slots), F32),
            pltpu.SemaphoreType.DMA((3,)),
            pltpu.SemaphoreType.DMA((windows, cell_width // chunk)),
            pltpu.SemaphoreType.DMA((windows + 1, count)),
            pltpu.SemaphoreType.DMA((windows + 1, count)),
        ],
        compiler_params=pltpu.CompilerParams(
            collective_id=0, has_side_effects=True, vmem_limit_bytes=12 * MIB
        ),
        cost_estimate=pl.CostEstimate(flops=2 * 10**9, bytes_accessed=MIB, transcendentals=0),
        name="observe",
    )(
        *(
            pltpu.with_memory_space_constraint(value, pltpu.HBM)
            for value in (anomalies, obs_cells, obs_counts.reshape(windows), obs_precision)
        )
    )
    partial, own = pl.pallas_call(
        transforms_kernel,
        out_shape=(
            jax.ShapeDtypeStruct((windows, members, members), F32),
            jax.ShapeDtypeStruct((members, members), BF16),
        ),
        in_specs=[smem, vmem, vmem],
        out_specs=(vmem, vmem),
        scratch_shapes=[pltpu.VMEM((windows, members, members), BF16)] * 2
        + [pltpu.VMEM((windows, members, members), F32)]
        + [pltpu.VMEM((windows, half, half), F32)] * 3,
        compiler_params=pltpu.CompilerParams(vmem_limit_bytes=16 * MIB),
        cost_estimate=pl.CostEstimate(flops=4 * 10**9, bytes_accessed=2 * MIB, transcendentals=0),
        name="transforms",
    )(inflation, gathered, gathered_weights)
    devices = lax.axis_size("tm")
    hops = pltpu.SemaphoreType.DMA((devices // 2, 3))
    later = pl.pallas_call(
        lambda *refs: suffix_kernel("tm", devices, *refs),
        out_shape=jax.ShapeDtypeStruct((members, members), F32),
        in_specs=[vmem],
        out_specs=vmem,
        scratch_shapes=[
            pltpu.VMEM((members, members), BF16),
            pltpu.VMEM((members, members), BF16),
            pltpu.VMEM((devices // 2, members, members), BF16),
            pltpu.SemaphoreType.DMA((2,)),
        ]
        + [hops] * 4,
        compiler_params=pltpu.CompilerParams(
            collective_id=1, has_side_effects=True, vmem_limit_bytes=8 * MIB
        ),
        cost_estimate=pl.CostEstimate(flops=2 * 10**9, bytes_accessed=MIB, transcendentals=0),
        name="suffix",
    )(own)
    flat = anomalies.reshape(windows, fields * cell_width, members)
    tile = min(512, cell_width)
    result = pl.pallas_call(
        apply_kernel,
        out_shape=jax.ShapeDtypeStruct(flat.shape, BF16),
        in_specs=[vmem, vmem, vmem],
        out_specs=hbm,
        scratch_shapes=[
            pltpu.VMEM((windows, fields * cell_width // tile, tile, members), BF16),
            pltpu.SemaphoreType.DMA((windows, fields * cell_width // tile)),
        ],
        compiler_params=pltpu.CompilerParams(vmem_limit_bytes=16 * MIB),
        name="apply",
    )(flat, later, partial)
    return result.reshape(anomalies.shape)


def solution(mesh):
    placed = (
        P("tm", None, "cell", None),
        P("tm", "cell"),
        P("tm", "cell"),
        P("tm", "cell"),
        P("tm"),
    )
    return jax.shard_map(
        local, mesh=mesh, in_specs=placed, out_specs=P("tm", None, "cell", None), check_vma=False
    )
```

```python
import jax
import jax.numpy as jnp
from jax import lax
from jax.experimental import pallas as pl
from jax.experimental.pallas import tpu as pltpu
from jax.sharding import PartitionSpec as P

F32 = jnp.float32
BF16 = jnp.bfloat16
SPREAD_GAIN = 1.9
SETTLED = 2.5e-3
MIB = 1 << 20


def dot_any(left, right, dims):
    return lax.dot_general(left, right, (dims, ((), ())), preferred_element_type=F32)


def halves(value):
    high = value.astype(BF16)
    return high, (value - high.astype(F32)).astype(BF16)


def dot_three(left, right, dims=((1,), (0,))):
    lh, ll = halves(left)
    rh, rl = halves(right)
    return dot_any(lh, rh, dims) + (dot_any(lh, rl, dims) + dot_any(ll, rh, dims))


def dot_full(left, right, dims=((1,), (0,))):
    return lax.dot_general(
        left, right, (dims, ((), ())), precision=lax.Precision.HIGHEST, preferred_element_type=F32
    )


def eliminate(matrices):
    size = matrices[0].shape[0]
    groups = size // 8
    lane = lax.broadcasted_iota(jnp.int32, (8, size), 1)
    sub = lax.broadcasted_iota(jnp.int32, (8, size), 0)
    work = [[m[8 * g : 8 * g + 8, :] for g in range(groups)] for m in matrices]
    for k in range(0, size, 2):
        g, r = divmod(k, 8)
        first_lane, second_lane = lane == k, lane == k + 1
        either = first_lane | second_lane
        for rows in work:
            own = rows[g]
            near = jnp.broadcast_to(own[:, k : k + 1], (8, size))
            far = jnp.broadcast_to(own[:, k + 1 : k + 2], (8, size))
            d0 = jnp.broadcast_to(near[r : r + 1, :], (8, size))
            m = jnp.broadcast_to(near[r + 1 : r + 2, :], (8, size))
            e = jnp.broadcast_to(far[r + 1 : r + 2, :], (8, size))
            row0 = jnp.broadcast_to(own[r : r + 1, :], (8, size))
            row1 = jnp.broadcast_to(own[r + 1 : r + 2, :], (8, size))
            i0 = 1.0 / d0
            step = m * i0
            i1 = 1.0 / (e - step * m)
            row0_one = jnp.where(first_lane, 1.0, row0)
            row1_mid = jnp.where(first_lane, 0.0, row1) - step * row0_one
            p0 = jnp.where(second_lane, 0.0, row0_one) * i0
            p1 = jnp.where(second_lane, 1.0, row1_mid) * i1
            for i in range(g, groups):
                if i == g:
                    c0, c1 = near, far
                else:
                    c0 = jnp.broadcast_to(rows[i][:, k : k + 1], (8, size))
                    c1 = jnp.broadcast_to(rows[i][:, k + 1 : k + 2], (8, size))
                c1 = c1 - c0 * step
                new = jnp.where(either, 0.0, rows[i]) - c0 * p0 - c1 * p1
                if i == g:
                    new = jnp.where(sub <= r, own, jnp.where(sub == r + 1, row1_mid, new))
                rows[i] = new
    results = []
    for rows in work:
        pieces = []
        for g in range(groups):
            row = sub + 8 * g
            pivot = jnp.sum(jnp.where(lane == row, rows[g], 0.0), axis=1, keepdims=True)
            unit = jnp.where(lane < row, rows[g], jnp.where(lane == row, 1.0, 0.0))
            pieces.append(unit * lax.rsqrt(pivot))
        results.append(jnp.concatenate(pieces, axis=0))
    return results


def lower_half(value, row, col):
    return jnp.where(row > col, value, jnp.where(row == col, 0.5 * value, 0.0))


def transforms_kernel(
    rho_ref, picked_ref, weight_ref, partial_ref, own_ref, high_ref, low_ref, x_ref, first_inv, second_inv, mid_ref
):
    blocks, windows, slots, members = picked_ref.shape
    slot_eye = (
        lax.broadcasted_iota(jnp.int32, (slots, slots), 0)
        == lax.broadcasted_iota(jnp.int32, (slots, slots), 1)
    )
    row = lax.broadcasted_iota(jnp.int32, (members, members), 0)
    col = lax.broadcasted_iota(jnp.int32, (members, members), 1)
    eye = row == col
    nn = ((1,), (0,))
    tn = ((0,), (0,))
    nt = ((1,), (1,))

    unit = jnp.where(eye, 1.0, 0.0)

    every = range(windows)

    def squares(changes):
        narrow = [change.astype(BF16) for change in changes]
        plain = [dot_any(n, n, nn) for n in narrow]
        crossed = [dot_any(n, n, nt) for n in narrow]
        return [p + lower_half(c, row, col) for p, c in zip(plain, crossed)]

    def correct(narrow_x, changes):
        steps = [(c - s).astype(BF16) for c, s in zip(changes, squares(changes))]
        moves = [dot_any(step, narrow_x[w], nn) for w, step in enumerate(steps)]
        for w in every:
            x_ref[w] -= moves[w]

    rows = [jnp.concatenate([picked_ref[n, w] for n in range(blocks)], axis=0) for w in every]
    columns = [
        jnp.concatenate(
            [
                jnp.sum(
                    jnp.where(slot_eye, weight_ref[n, w : w + 1, :], 0.0), axis=1, keepdims=True
                )
                for n in range(blocks)
            ],
            axis=0,
        )
        for w in every
    ]
    wide = [value.astype(F32) for value in rows]
    scaled = [wide[w] * columns[w] for w in every]
    scale_rows = [
        jnp.sqrt(1.0 / (jnp.sum(scaled[w] * wide[w], axis=0, keepdims=True) + F32(members - 1.0)))
        for w in every
    ]
    near_rows = [(wide[w] * (jnp.sqrt(columns[w]) * scale_rows[w])).astype(BF16) for w in every]
    offs = [jnp.where(eye, 0.0, dot_any(value, value, tn)) for value in near_rows]
    splits = [halves(value) for value in scaled]
    for w in every:
        system = dot_any(rows[w], splits[w][0], tn) + dot_any(rows[w], splits[w][1], tn)
        high_ref[w], low_ref[w] = halves(system + F32(members - 1.0) * unit)
    spreads = [
        jnp.sum(jnp.sum(off * off, axis=0, keepdims=True), axis=1, keepdims=True) for off in offs
    ]
    betas = [1.0 / (1.0 + SPREAD_GAIN * jnp.sqrt(spread * (1.0 / members))) for spread in spreads]
    changes = [
        jnp.where(row > col, beta * off, jnp.where(eye, 0.5 * (beta - 1.0), 0.0))
        for beta, off in zip(betas, offs)
    ]
    scales = [scale_rows[w] * jnp.sqrt(betas[w]) for w in every]

    for w, second in enumerate(squares(changes)):
        x_ref[w] = (unit - changes[w] + second) * scales[w]

    xh = [x_ref[w].astype(BF16) for w in every]
    left = [dot_any(xh[w], high_ref[w], nn).astype(BF16) for w in every]
    correct(xh, [lower_half(dot_any(left[w], xh[w], nt) - unit, row, col) for w in every])

    def refine(state):
        turn, _ = state
        worst = jnp.zeros((1, 1), F32)
        xs = [halves(x_ref[w]) for w in every]
        left = [
            dot_any(xs[w][0], high_ref[w], nn)
            + (dot_any(xs[w][0], low_ref[w], nn) + dot_any(xs[w][1], high_ref[w], nn))
            for w in every
        ]
        ls = [halves(value) for value in left]
        near = [
            dot_any(ls[w][0], xs[w][0], nt)
            + (dot_any(ls[w][0], xs[w][1], nt) + dot_any(ls[w][1], xs[w][0], nt))
            for w in every
        ]
        changes = [lower_half(value - unit, row, col) for value in near]
        for change in changes:
            size = jnp.sum(jnp.sum(change * change, axis=0, keepdims=True), axis=1, keepdims=True)
            worst = jnp.where(size <= worst, worst, size)
        correct([x[0] for x in xs], changes)
        return turn + 1, worst[0, 0]

    def again(state):
        turn, size = state
        return (turn < 8) & (size > SETTLED) & (size < 1.0)

    _, size = lax.while_loop(again, refine, refine((jnp.int32(0), F32(0.5))))

    @pl.when(jnp.logical_not(size <= SETTLED))
    def _():
        direct(high_ref, low_ref, partial_ref, x_ref, first_inv, second_inv, mid_ref)

    for w in range(windows):
        scale = rho_ref[w] * jnp.sqrt(F32(members - 1.0))
        partial_ref[w] = scale * x_ref[w]

    for turn in range(windows - 1):
        w = windows - 2 - turn
        partial_ref[w] = dot_three(partial_ref[w + 1], partial_ref[w])

    own_ref[...] = partial_ref[0].astype(BF16)


def direct(high_ref, low_ref, gram, x_ref, first_inv, second_inv, mid_ref):
    windows, members, _ = x_ref.shape
    half = members // 2
    nt = ((1,), (1,))

    for w in range(windows):
        gram[w] = high_ref[w].astype(F32) + low_ref[w].astype(F32)

    for w, value in enumerate(eliminate([gram[w, :half, :half] for w in range(windows)])):
        first_inv[w] = value

    @pl.loop(0, windows)
    def _(w):
        lower = dot_full(gram[w, half:, :half], first_inv[w], nt)
        gram[w, half:, half:] -= dot_full(lower, lower, nt)
        mid_ref[w] = dot_full(lower, first_inv[w])

    for w, value in enumerate(eliminate([gram[w, half:, half:] for w in range(windows)])):
        second_inv[w] = value

    @pl.loop(0, windows)
    def _(w):
        x_ref[w, :half, :half] = first_inv[w]
        x_ref[w, :half, half:] = jnp.zeros((half, half), F32)
        x_ref[w, half:, :half] = -dot_full(second_inv[w], mid_ref[w])
        x_ref[w, half:, half:] = second_inv[w]


def suffix_kernel(
    axis, count, own_ref, later_ref, other, mine, wholes, pair_sem, send_sem, recv_sem, pass_send, pass_recv
):
    members = own_ref.shape[0]
    half = members // 2
    chips = count // 2
    me = lax.axis_index(axis)
    chip, core = lax.div(me, 2), lax.rem(me, 2)
    partner = me + 1 - 2 * core
    nn = ((1,), (0,))
    left, right = pl.ds(0, half), pl.ds(half, half)
    split = half + half // 2
    pieces = (
        (pl.ds(0, split), left),
        (pl.ds(split, members - split), left),
        (right, right),
    )
    owned = ((0,), (1, 2))

    for shift in range(1, chips):
        wholes[shift, :half, half:] = jnp.zeros((half, half), BF16)
    barrier = pltpu.get_barrier_semaphore()

    def greet(device):
        pl.semaphore_signal(
            barrier, inc=1, device_id={axis: device}, device_id_type=pl.DeviceIdType.MESH
        )

    greet(partner)
    for shift in range(1, chips):
        greet(lax.rem(me + 2 * shift, count))
    pl.semaphore_wait(barrier, chips)

    def copy_to(device, source, target, send, recv):
        return pltpu.make_async_remote_copy(
            src_ref=source,
            dst_ref=target,
            send_sem=send,
            recv_sem=recv,
            device_id={axis: device},
            device_id_type=pl.DeviceIdType.MESH,
        )

    def down(shift, p):
        rows, cols = pieces[p]
        return copy_to(
            lax.rem(me + count - 2 * shift, count),
            mine.at[rows, cols],
            wholes.at[shift, rows, cols],
            send_sem.at[shift, p],
            recv_sem.at[shift, p],
        )

    def across(shift, p):
        rows, cols = pieces[p]
        place = wholes.at[shift, rows, cols]
        return copy_to(partner, place, place, pass_send.at[shift, p], pass_recv.at[shift, p])

    pair = copy_to(partner, own_ref, other, pair_sem.at[0], pair_sem.at[1])
    pair.start()
    pair.wait()
    first = core == 0
    low_rows, high_rows = own_ref[...], other[...]
    later_left = jnp.where(first, high_rows, low_rows)
    later_right = jnp.where(first, low_rows, high_rows)
    mine[...] = dot_any(later_left, later_right, nn).astype(BF16)

    for k in range(2):
        for shift in range(chips - 1, 0, -1):

            @pl.when((core == k) & (chip >= shift))
            def _():
                for p in owned[k]:
                    down(shift, p).start()

    for k in range(2):
        for shift in range(1, chips):

            @pl.when((core == k) & (chip + shift < chips))
            def _():
                for p in owned[k]:
                    down(shift, p).wait_recv()
                    across(shift, p).start()

    row = lax.broadcasted_iota(jnp.int32, (members, members), 0)
    col = lax.broadcasted_iota(jnp.int32, (members, members), 1)
    later_ref[...] = jnp.where(first, high_rows.astype(F32), jnp.where(row == col, 1.0, 0.0))
    for shift in range(1, chips):

        @pl.when(chip + shift < chips)
        def _():
            for k in range(2):

                @pl.when(core == k)
                def _():
                    for p in owned[1 - k]:
                        across(shift, p).wait_recv()

            high, low = halves(later_ref[...])
            whole = wholes[shift]
            later_ref[...] = dot_any(whole, high, nn) + dot_any(whole, low, nn)

    for k in range(2):
        for shift in range(1, chips):

            @pl.when((core == k) & (chip >= shift))
            def _():
                for p in owned[k]:
                    down(shift, p).wait_send()

            @pl.when((core == k) & (chip + shift < chips))
            def _():
                for p in owned[k]:
                    across(shift, p).wait_send()


def observe_kernel(axis, count, chunk, field_ref, cells_hbm, counts_hbm, precision_hbm,
    rows_ref, weights_ref, dens, cells_ref, counts_ref, precision_ref, small_sem, load_sem, send_sem, recv_sem):
    windows, slots = cells_ref.shape
    depth = dens.shape[1]
    pieces = depth // chunk
    me = lax.axis_index(axis)

    def load_of(w, piece):
        span = pl.ds(piece * chunk, chunk)
        return pltpu.make_async_copy(
            field_ref.at[w, 0, span, :], dens.at[w, span, :], load_sem.at[w, piece]
        )

    small = [
        pltpu.make_async_copy(source, target, small_sem.at[i])
        for i, (source, target) in enumerate(
            ((cells_hbm, cells_ref), (counts_hbm, counts_ref), (precision_hbm, precision_ref))
        )
    ]
    for copy in small:
        copy.start()
    for w in range(windows):
        for piece in range(pieces):
            load_of(w, piece).start()
    barrier = pltpu.get_barrier_semaphore()
    for shift in range(1, count):
        pl.semaphore_signal(
            barrier,
            inc=1,
            device_id={axis: lax.rem(me + shift, count)},
            device_id_type=pl.DeviceIdType.MESH,
        )

    def copy_of(shift, item, source, target):
        return pltpu.make_async_remote_copy(
            src_ref=source,
            dst_ref=target,
            send_sem=send_sem.at[item, shift],
            recv_sem=recv_sem.at[item, shift],
            device_id={axis: lax.rem(me + count - shift, count)},
            device_id_type=pl.DeviceIdType.MESH,
        )

    def rows_copy(shift, w):
        return copy_of(shift, w, rows_ref.at[me, w], rows_ref.at[me, w])

    def weights_copy(shift):
        return copy_of(shift, windows, weights_ref.at[me], weights_ref.at[me])

    for copy in small:
        copy.wait()
    slot = lax.broadcasted_iota(jnp.int32, (windows, slots), 1)
    window = lax.broadcasted_iota(jnp.int32, (windows, slots), 0)
    counts = jnp.zeros((windows, slots), jnp.int32)
    for w in range(windows):
        counts = jnp.where(window == w, counts_ref[w], counts)
    weights_ref[me] = jnp.where(slot < counts, precision_ref[...], 0.0)
    slot_eye = (
        lax.broadcasted_iota(jnp.int32, (slots, slots), 0)
        == lax.broadcasted_iota(jnp.int32, (slots, slots), 1)
    )
    place = lax.broadcasted_iota(jnp.int32, (slots, chunk), 1)
    offsets = (cells_ref[...] - me * depth).astype(F32)
    columns = [
        jnp.sum(jnp.where(slot_eye, offsets[w : w + 1, :], 0.0), axis=1, keepdims=True).astype(
            jnp.int32
        )
        for w in range(windows)
    ]
    for w in range(windows):
        total = jnp.zeros((slots, dens.shape[2]), F32)
        for piece in range(pieces):
            hit = jnp.where(place + piece * chunk == columns[w], 1.0, 0.0).astype(BF16)
            load_of(w, piece).wait()
            total += dot_any(hit, dens[w, pl.ds(piece * chunk, chunk), :], ((1,), (0,)))
        rows_ref[me, w] = total.astype(BF16)
        if w == 0:
            pl.semaphore_wait(barrier, count - 1)
            for shift in range(1, count):
                weights_copy(shift).start()
        for far in range(count - 1, 0, -1):
            pl.when(me >= far)(rows_copy(far, w).start)
            pl.when(me + far < count)(rows_copy(count - far, w).start)
    for shift in range(1, count):
        weights_copy(shift).wait()
        for w in range(windows):
            rows_copy(shift, w).wait()


def apply_kernel(field_ref, later_ref, partial_ref, out_ref, stage, sems):
    windows, height, _ = field_ref.shape
    tile = stage.shape[2]
    tiles = height // tile
    nn = ((1,), (0,))

    def out_of(w, t):
        return pltpu.make_async_copy(
            stage.at[w, t], out_ref.at[w, pl.ds(t * tile, tile), :], sems.at[w, t]
        )

    high, low = halves(later_ref[...])
    parts = [halves(partial_ref[w]) for w in range(windows)]
    weights = [
        (
            dot_any(high, parts[w][0], nn)
            + (dot_any(high, parts[w][1], nn) + dot_any(low, parts[w][0], nn))
        ).astype(BF16)
        for w in range(windows)
    ]
    for w in range(windows):
        for t in range(tiles):
            stage[w, t] = dot_any(
                field_ref[w, pl.ds(t * tile, tile), :], weights[w], ((1,), (1,))
            ).astype(BF16)
            out_of(w, t).start()
    for w in range(windows):
        for t in range(tiles):
            out_of(w, t).wait()


def local(anomalies, obs_cells, obs_counts, obs_precision, inflation):
    windows, fields, cell_width, members = anomalies.shape
    half = members // 2
    slots = obs_cells.shape[1]
    count = lax.axis_size("cell")
    chunk = min(1024, cell_width)
    vmem = pl.BlockSpec(memory_space=pltpu.VMEM)
    smem = pl.BlockSpec(memory_space=pltpu.SMEM)
    hbm = pl.BlockSpec(memory_space=pltpu.HBM)
    gathered, gathered_weights = pl.pallas_call(
        lambda *refs: observe_kernel("cell", count, chunk, *refs),
        out_shape=(
            jax.ShapeDtypeStruct((count, windows, slots, members), BF16),
            jax.ShapeDtypeStruct((count, windows, slots), F32),
        ),
        in_specs=[hbm] * 4,
        out_specs=(vmem, vmem),
        scratch_shapes=[
            pltpu.VMEM((windows, cell_width, members), BF16),
            pltpu.VMEM((windows, slots), jnp.int32),
            pltpu.SMEM((windows,), jnp.int32),
            pltpu.VMEM((windows, slots), F32),
            pltpu.SemaphoreType.DMA((3,)),
            pltpu.SemaphoreType.DMA((windows, cell_width // chunk)),
            pltpu.SemaphoreType.DMA((windows + 1, count)),
            pltpu.SemaphoreType.DMA((windows + 1, count)),
        ],
        compiler_params=pltpu.CompilerParams(
            collective_id=0, has_side_effects=True, vmem_limit_bytes=12 * MIB
        ),
        cost_estimate=pl.CostEstimate(flops=2 * 10**9, bytes_accessed=MIB, transcendentals=0),
        name="observe",
    )(
        *(
            pltpu.with_memory_space_constraint(value, pltpu.HBM)
            for value in (anomalies, obs_cells, obs_counts.reshape(windows), obs_precision)
        )
    )
    partial, own = pl.pallas_call(
        transforms_kernel,
        out_shape=(
            jax.ShapeDtypeStruct((windows, members, members), F32),
            jax.ShapeDtypeStruct((members, members), BF16),
        ),
        in_specs=[smem, vmem, vmem],
        out_specs=(vmem, vmem),
        scratch_shapes=[pltpu.VMEM((windows, members, members), BF16)] * 2
        + [pltpu.VMEM((windows, members, members), F32)]
        + [pltpu.VMEM((windows, half, half), F32)] * 3,
        compiler_params=pltpu.CompilerParams(vmem_limit_bytes=16 * MIB),
        cost_estimate=pl.CostEstimate(flops=4 * 10**9, bytes_accessed=2 * MIB, transcendentals=0),
        name="transforms",
    )(inflation, gathered, gathered_weights)
    devices = lax.axis_size("tm")
    hops = pltpu.SemaphoreType.DMA((devices // 2, 3))
    later = pl.pallas_call(
        lambda *refs: suffix_kernel("tm", devices, *refs),
        out_shape=jax.ShapeDtypeStruct((members, members), F32),
        in_specs=[vmem],
        out_specs=vmem,
        scratch_shapes=[
            pltpu.VMEM((members, members), BF16),
            pltpu.VMEM((members, members), BF16),
            pltpu.VMEM((devices // 2, members, members), BF16),
            pltpu.SemaphoreType.DMA((2,)),
        ]
        + [hops] * 4,
        compiler_params=pltpu.CompilerParams(
            collective_id=1, has_side_effects=True, vmem_limit_bytes=8 * MIB
        ),
        cost_estimate=pl.CostEstimate(flops=2 * 10**9, bytes_accessed=MIB, transcendentals=0),
        name="suffix",
    )(own)
    flat = anomalies.reshape(windows, fields * cell_width, members)
    tile = min(512, cell_width)
    result = pl.pallas_call(
        apply_kernel,
        out_shape=jax.ShapeDtypeStruct(flat.shape, BF16),
        in_specs=[vmem, vmem, vmem],
        out_specs=hbm,
        scratch_shapes=[
            pltpu.VMEM((windows, fields * cell_width // tile, tile, members), BF16),
            pltpu.SemaphoreType.DMA((windows, fields * cell_width // tile)),
        ],
        compiler_params=pltpu.CompilerParams(vmem_limit_bytes=16 * MIB),
        name="apply",
    )(flat, later, partial)
    return result.reshape(anomalies.shape)


def solution(mesh):
    placed = (
        P("tm", None, "cell", None),
        P("tm", "cell"),
        P("tm", "cell"),
        P("tm", "cell"),
        P("tm"),
    )
    return jax.shard_map(
        local, mesh=mesh, in_specs=placed, out_specs=P("tm", None, "cell", None), check_vma=False
    )
```

```python
import jax
import jax.numpy as jnp
from jax import lax
from jax.experimental import pallas as pl
from jax.experimental.pallas import tpu as pltpu
from jax.sharding import PartitionSpec as P

F32 = jnp.float32
BF16 = jnp.bfloat16
SPREAD_GAIN = 1.9
SETTLED = 2.5e-3
MIB = 1 << 20


def dot_any(left, right, dims):
    return lax.dot_general(left, right, (dims, ((), ())), preferred_element_type=F32)


def halves(value):
    high = value.astype(BF16)
    return high, (value - high.astype(F32)).astype(BF16)


def dot_three(left, right, dims=((1,), (0,))):
    lh, ll = halves(left)
    rh, rl = halves(right)
    return dot_any(lh, rh, dims) + (dot_any(lh, rl, dims) + dot_any(ll, rh, dims))


def dot_full(left, right, dims=((1,), (0,))):
    return lax.dot_general(
        left, right, (dims, ((), ())), precision=lax.Precision.HIGHEST, preferred_element_type=F32
    )


def eliminate(matrices):
    size = matrices[0].shape[0]
    groups = size // 8
    lane = lax.broadcasted_iota(jnp.int32, (8, size), 1)
    sub = lax.broadcasted_iota(jnp.int32, (8, size), 0)
    work = [[m[8 * g : 8 * g + 8, :] for g in range(groups)] for m in matrices]
    for k in range(0, size, 2):
        g, r = divmod(k, 8)
        first_lane, second_lane = lane == k, lane == k + 1
        either = first_lane | second_lane
        for rows in work:
            own = rows[g]
            near = jnp.broadcast_to(own[:, k : k + 1], (8, size))
            far = jnp.broadcast_to(own[:, k + 1 : k + 2], (8, size))
            d0 = jnp.broadcast_to(near[r : r + 1, :], (8, size))
            m = jnp.broadcast_to(near[r + 1 : r + 2, :], (8, size))
            e = jnp.broadcast_to(far[r + 1 : r + 2, :], (8, size))
            row0 = jnp.broadcast_to(own[r : r + 1, :], (8, size))
            row1 = jnp.broadcast_to(own[r + 1 : r + 2, :], (8, size))
            i0 = 1.0 / d0
            step = m * i0
            i1 = 1.0 / (e - step * m)
            row0_one = jnp.where(first_lane, 1.0, row0)
            row1_mid = jnp.where(first_lane, 0.0, row1) - step * row0_one
            p0 = jnp.where(second_lane, 0.0, row0_one) * i0
            p1 = jnp.where(second_lane, 1.0, row1_mid) * i1
            for i in range(g, groups):
                if i == g:
                    c0, c1 = near, far
                else:
                    c0 = jnp.broadcast_to(rows[i][:, k : k + 1], (8, size))
                    c1 = jnp.broadcast_to(rows[i][:, k + 1 : k + 2], (8, size))
                c1 = c1 - c0 * step
                new = jnp.where(either, 0.0, rows[i]) - c0 * p0 - c1 * p1
                if i == g:
                    new = jnp.where(sub <= r, own, jnp.where(sub == r + 1, row1_mid, new))
                rows[i] = new
    results = []
    for rows in work:
        pieces = []
        for g in range(groups):
            row = sub + 8 * g
            pivot = jnp.sum(jnp.where(lane == row, rows[g], 0.0), axis=1, keepdims=True)
            unit = jnp.where(lane < row, rows[g], jnp.where(lane == row, 1.0, 0.0))
            pieces.append(unit * lax.rsqrt(pivot))
        results.append(jnp.concatenate(pieces, axis=0))
    return results


def lower_half(value, row, col):
    return jnp.where(row > col, value, jnp.where(row == col, 0.5 * value, 0.0))


def transforms_kernel(
    rho_ref, picked_ref, weight_ref, partial_ref, own_ref, high_ref, low_ref, x_ref, first_inv, second_inv, mid_ref
):
    blocks, windows, slots, members = picked_ref.shape
    slot_eye = (
        lax.broadcasted_iota(jnp.int32, (slots, slots), 0)
        == lax.broadcasted_iota(jnp.int32, (slots, slots), 1)
    )
    row = lax.broadcasted_iota(jnp.int32, (members, members), 0)
    col = lax.broadcasted_iota(jnp.int32, (members, members), 1)
    eye = row == col
    nn = ((1,), (0,))
    tn = ((0,), (0,))
    nt = ((1,), (1,))

    unit = jnp.where(eye, 1.0, 0.0)

    every = range(windows)

    def squares(changes):
        narrow = [change.astype(BF16) for change in changes]
        plain = [dot_any(n, n, nn) for n in narrow]
        crossed = [dot_any(n, n, nt) for n in narrow]
        return [p + lower_half(c, row, col) for p, c in zip(plain, crossed)]

    def correct(narrow_x, changes):
        steps = [(c - s).astype(BF16) for c, s in zip(changes, squares(changes))]
        moves = [dot_any(step, narrow_x[w], nn) for w, step in enumerate(steps)]
        for w in every:
            x_ref[w] -= moves[w]

    rows = [jnp.concatenate([picked_ref[n, w] for n in range(blocks)], axis=0) for w in every]
    columns = [
        jnp.concatenate(
            [
                jnp.sum(
                    jnp.where(slot_eye, weight_ref[n, w : w + 1, :], 0.0), axis=1, keepdims=True
                )
                for n in range(blocks)
            ],
            axis=0,
        )
        for w in every
    ]
    wide = [value.astype(F32) for value in rows]
    scaled = [wide[w] * columns[w] for w in every]
    scale_rows = [
        jnp.sqrt(1.0 / (jnp.sum(scaled[w] * wide[w], axis=0, keepdims=True) + F32(members - 1.0)))
        for w in every
    ]
    near_rows = [(wide[w] * (jnp.sqrt(columns[w]) * scale_rows[w])).astype(BF16) for w in every]
    offs = [jnp.where(eye, 0.0, dot_any(value, value, tn)) for value in near_rows]
    splits = [halves(value) for value in scaled]
    for w in every:
        system = dot_any(rows[w], splits[w][0], tn) + dot_any(rows[w], splits[w][1], tn)
        high_ref[w], low_ref[w] = halves(system + F32(members - 1.0) * unit)
    spreads = [
        jnp.sum(jnp.sum(off * off, axis=0, keepdims=True), axis=1, keepdims=True) for off in offs
    ]
    betas = [1.0 / (1.0 + SPREAD_GAIN * jnp.sqrt(spread * (1.0 / members))) for spread in spreads]
    changes = [
        jnp.where(row > col, beta * off, jnp.where(eye, 0.5 * (beta - 1.0), 0.0))
        for beta, off in zip(betas, offs)
    ]
    scales = [scale_rows[w] * jnp.sqrt(betas[w]) for w in every]

    for w, second in enumerate(squares(changes)):
        x_ref[w] = (unit - changes[w] + second) * scales[w]

    xh = [x_ref[w].astype(BF16) for w in every]
    left = [dot_any(xh[w], high_ref[w], nn).astype(BF16) for w in every]
    correct(xh, [lower_half(dot_any(left[w], xh[w], nt) - unit, row, col) for w in every])

    def refine(state):
        turn, _ = state
        worst = jnp.zeros((1, 1), F32)
        xs = [halves(x_ref[w]) for w in every]
        left = [
            dot_any(xs[w][0], high_ref[w], nn)
            + (dot_any(xs[w][0], low_ref[w], nn) + dot_any(xs[w][1], high_ref[w], nn))
            for w in every
        ]
        ls = [halves(value) for value in left]
        near = [
            dot_any(ls[w][0], xs[w][0], nt)
            + (dot_any(ls[w][0], xs[w][1], nt) + dot_any(ls[w][1], xs[w][0], nt))
            for w in every
        ]
        changes = [lower_half(value - unit, row, col) for value in near]
        for change in changes:
            size = jnp.sum(jnp.sum(change * change, axis=0, keepdims=True), axis=1, keepdims=True)
            worst = jnp.where(size <= worst, worst, size)
        correct([x[0] for x in xs], changes)
        return turn + 1, worst[0, 0]

    def again(state):
        turn, size = state
        return (turn < 8) & (size > SETTLED) & (size < 1.0)

    _, size = lax.while_loop(again, refine, refine((jnp.int32(0), F32(0.5))))

    @pl.when(jnp.logical_not(size <= SETTLED))
    def _():
        direct(high_ref, low_ref, partial_ref, x_ref, first_inv, second_inv, mid_ref)

    for w in range(windows):
        scale = rho_ref[w] * jnp.sqrt(F32(members - 1.0))
        partial_ref[w] = scale * x_ref[w]

    for turn in range(windows - 1):
        w = windows - 2 - turn
        partial_ref[w] = dot_three(partial_ref[w + 1], partial_ref[w])

    own_ref[...] = partial_ref[0].astype(BF16)


def direct(high_ref, low_ref, gram, x_ref, first_inv, second_inv, mid_ref):
    windows, members, _ = x_ref.shape
    half = members // 2
    nt = ((1,), (1,))

    for w in range(windows):
        gram[w] = high_ref[w].astype(F32) + low_ref[w].astype(F32)

    for w, value in enumerate(eliminate([gram[w, :half, :half] for w in range(windows)])):
        first_inv[w] = value

    @pl.loop(0, windows)
    def _(w):
        lower = dot_full(gram[w, half:, :half], first_inv[w], nt)
        gram[w, half:, half:] -= dot_full(lower, lower, nt)
        mid_ref[w] = dot_full(lower, first_inv[w])

    for w, value in enumerate(eliminate([gram[w, half:, half:] for w in range(windows)])):
        second_inv[w] = value

    @pl.loop(0, windows)
    def _(w):
        x_ref[w, :half, :half] = first_inv[w]
        x_ref[w, :half, half:] = jnp.zeros((half, half), F32)
        x_ref[w, half:, :half] = -dot_full(second_inv[w], mid_ref[w])
        x_ref[w, half:, half:] = second_inv[w]


def suffix_kernel(
    axis, count, own_ref, partial_ref, weights_ref, values, other, mine, wholes, pair_sem, send_sem, recv_sem, pass_send, pass_recv
):
    members = own_ref.shape[0]
    half = members // 2
    chips = count // 2
    me = lax.axis_index(axis)
    chip, core = lax.div(me, 2), lax.rem(me, 2)
    partner = me + 1 - 2 * core
    nn = ((1,), (0,))
    left, right = pl.ds(0, half), pl.ds(half, half)
    split = half + half // 2
    pieces = (
        (pl.ds(0, split), left),
        (pl.ds(split, members - split), left),
        (right, right),
    )
    owned = ((0,), (1, 2))

    for shift in range(1, chips):
        wholes[shift, :half, half:] = jnp.zeros((half, half), BF16)
    barrier = pltpu.get_barrier_semaphore()

    def greet(device):
        pl.semaphore_signal(
            barrier, inc=1, device_id={axis: device}, device_id_type=pl.DeviceIdType.MESH
        )

    greet(partner)
    for shift in range(1, chips):
        greet(lax.rem(me + 2 * shift, count))
    pl.semaphore_wait(barrier, chips)

    def copy_to(device, source, target, send, recv):
        return pltpu.make_async_remote_copy(
            src_ref=source,
            dst_ref=target,
            send_sem=send,
            recv_sem=recv,
            device_id={axis: device},
            device_id_type=pl.DeviceIdType.MESH,
        )

    def down(shift, p):
        rows, cols = pieces[p]
        return copy_to(
            lax.rem(me + count - 2 * shift, count),
            mine.at[rows, cols],
            wholes.at[shift, rows, cols],
            send_sem.at[shift, p],
            recv_sem.at[shift, p],
        )

    def across(shift, p):
        rows, cols = pieces[p]
        place = wholes.at[shift, rows, cols]
        return copy_to(partner, place, place, pass_send.at[shift, p], pass_recv.at[shift, p])

    pair = copy_to(partner, own_ref, other, pair_sem.at[0], pair_sem.at[1])
    pair.start()
    pair.wait()
    first = core == 0
    low_rows, high_rows = own_ref[...], other[...]
    later_left = jnp.where(first, high_rows, low_rows)
    later_right = jnp.where(first, low_rows, high_rows)
    mine[...] = dot_any(later_left, later_right, nn).astype(BF16)

    for k in range(2):
        for shift in range(chips - 1, 0, -1):

            @pl.when((core == k) & (chip >= shift))
            def _():
                for p in owned[k]:
                    down(shift, p).start()

    every = range(partial_ref.shape[0])

    def multiplied(whole, source):
        split = [halves(source[w]) for w in every]
        for w, (high, low) in enumerate(split):
            values[w] = dot_any(whole, high, nn) + dot_any(whole, low, nn)

    @pl.when(first)
    def _():
        multiplied(other[...], partial_ref)

    @pl.when(core == 1)
    def _():
        values[...] = partial_ref[...]

    for k in range(2):
        for shift in range(1, chips):

            @pl.when((core == k) & (chip + shift < chips))
            def _():
                for p in owned[k]:
                    down(shift, p).wait_recv()
                    across(shift, p).start()

    for shift in range(1, chips):

        @pl.when(chip + shift < chips)
        def _():
            for k in range(2):

                @pl.when(core == k)
                def _():
                    for p in owned[1 - k]:
                        across(shift, p).wait_recv()

            multiplied(wholes[shift], values)

    weights_ref[...] = values[...].astype(BF16)

    for k in range(2):
        for shift in range(1, chips):

            @pl.when((core == k) & (chip >= shift))
            def _():
                for p in owned[k]:
                    down(shift, p).wait_send()

            @pl.when((core == k) & (chip + shift < chips))
            def _():
                for p in owned[k]:
                    across(shift, p).wait_send()


def observe_kernel(axis, count, chunk, field_ref, cells_hbm, counts_hbm, precision_hbm,
    rows_ref, weights_ref, dens, cells_ref, counts_ref, precision_ref, small_sem, load_sem, send_sem, recv_sem):
    windows, slots = cells_ref.shape
    depth = dens.shape[1]
    pieces = depth // chunk
    me = lax.axis_index(axis)

    def load_of(w, piece):
        span = pl.ds(piece * chunk, chunk)
        return pltpu.make_async_copy(
            field_ref.at[w, 0, span, :], dens.at[w, span, :], load_sem.at[w, piece]
        )

    small = [
        pltpu.make_async_copy(source, target, small_sem.at[i])
        for i, (source, target) in enumerate(
            ((cells_hbm, cells_ref), (counts_hbm, counts_ref), (precision_hbm, precision_ref))
        )
    ]
    for copy in small:
        copy.start()
    for w in range(windows):
        for piece in range(pieces):
            load_of(w, piece).start()
    barrier = pltpu.get_barrier_semaphore()
    for shift in range(1, count):
        pl.semaphore_signal(
            barrier,
            inc=1,
            device_id={axis: lax.rem(me + shift, count)},
            device_id_type=pl.DeviceIdType.MESH,
        )

    def copy_of(shift, item, source, target):
        return pltpu.make_async_remote_copy(
            src_ref=source,
            dst_ref=target,
            send_sem=send_sem.at[item, shift],
            recv_sem=recv_sem.at[item, shift],
            device_id={axis: lax.rem(me + count - shift, count)},
            device_id_type=pl.DeviceIdType.MESH,
        )

    def rows_copy(shift, w):
        return copy_of(shift, w, rows_ref.at[me, w], rows_ref.at[me, w])

    def weights_copy(shift):
        return copy_of(shift, windows, weights_ref.at[me], weights_ref.at[me])

    for copy in small:
        copy.wait()
    slot = lax.broadcasted_iota(jnp.int32, (windows, slots), 1)
    window = lax.broadcasted_iota(jnp.int32, (windows, slots), 0)
    counts = jnp.zeros((windows, slots), jnp.int32)
    for w in range(windows):
        counts = jnp.where(window == w, counts_ref[w], counts)
    weights_ref[me] = jnp.where(slot < counts, precision_ref[...], 0.0)
    slot_eye = (
        lax.broadcasted_iota(jnp.int32, (slots, slots), 0)
        == lax.broadcasted_iota(jnp.int32, (slots, slots), 1)
    )
    place = lax.broadcasted_iota(jnp.int32, (slots, chunk), 1)
    offsets = (cells_ref[...] - me * depth).astype(F32)
    columns = [
        jnp.sum(jnp.where(slot_eye, offsets[w : w + 1, :], 0.0), axis=1, keepdims=True).astype(
            jnp.int32
        )
        for w in range(windows)
    ]
    for w in range(windows):
        total = jnp.zeros((slots, dens.shape[2]), F32)
        for piece in range(pieces):
            hit = jnp.where(place + piece * chunk == columns[w], 1.0, 0.0).astype(BF16)
            load_of(w, piece).wait()
            total += dot_any(hit, dens[w, pl.ds(piece * chunk, chunk), :], ((1,), (0,)))
        rows_ref[me, w] = total.astype(BF16)
        if w == 0:
            pl.semaphore_wait(barrier, count - 1)
            for shift in range(1, count):
                weights_copy(shift).start()
        for far in range(count - 1, 0, -1):
            pl.when(me >= far)(rows_copy(far, w).start)
            pl.when(me + far < count)(rows_copy(count - far, w).start)
    for shift in range(1, count):
        weights_copy(shift).wait()
        for w in range(windows):
            rows_copy(shift, w).wait()


def apply_kernel(field_ref, weights_ref, out_ref, stage, sems):
    windows, height, _ = field_ref.shape
    tile = stage.shape[2]
    tiles = height // tile

    def out_of(w, t):
        return pltpu.make_async_copy(
            stage.at[w, t], out_ref.at[w, pl.ds(t * tile, tile), :], sems.at[w, t]
        )

    for w in range(windows):
        weight = weights_ref[w]
        for t in range(tiles):
            stage[w, t] = dot_any(
                field_ref[w, pl.ds(t * tile, tile), :], weight, ((1,), (1,))
            ).astype(BF16)
            out_of(w, t).start()
    for w in range(windows):
        for t in range(tiles):
            out_of(w, t).wait()


def local(anomalies, obs_cells, obs_counts, obs_precision, inflation):
    windows, fields, cell_width, members = anomalies.shape
    half = members // 2
    slots = obs_cells.shape[1]
    count = lax.axis_size("cell")
    chunk = min(1024, cell_width)
    vmem = pl.BlockSpec(memory_space=pltpu.VMEM)
    smem = pl.BlockSpec(memory_space=pltpu.SMEM)
    hbm = pl.BlockSpec(memory_space=pltpu.HBM)
    gathered, gathered_weights = pl.pallas_call(
        lambda *refs: observe_kernel("cell", count, chunk, *refs),
        out_shape=(
            jax.ShapeDtypeStruct((count, windows, slots, members), BF16),
            jax.ShapeDtypeStruct((count, windows, slots), F32),
        ),
        in_specs=[hbm] * 4,
        out_specs=(vmem, vmem),
        scratch_shapes=[
            pltpu.VMEM((windows, cell_width, members), BF16),
            pltpu.VMEM((windows, slots), jnp.int32),
            pltpu.SMEM((windows,), jnp.int32),
            pltpu.VMEM((windows, slots), F32),
            pltpu.SemaphoreType.DMA((3,)),
            pltpu.SemaphoreType.DMA((windows, cell_width // chunk)),
            pltpu.SemaphoreType.DMA((windows + 1, count)),
            pltpu.SemaphoreType.DMA((windows + 1, count)),
        ],
        compiler_params=pltpu.CompilerParams(
            collective_id=0, has_side_effects=True, vmem_limit_bytes=12 * MIB
        ),
        cost_estimate=pl.CostEstimate(flops=2 * 10**9, bytes_accessed=MIB, transcendentals=0),
        name="observe",
    )(
        *(
            pltpu.with_memory_space_constraint(value, pltpu.HBM)
            for value in (anomalies, obs_cells, obs_counts.reshape(windows), obs_precision)
        )
    )
    partial, own = pl.pallas_call(
        transforms_kernel,
        out_shape=(
            jax.ShapeDtypeStruct((windows, members, members), F32),
            jax.ShapeDtypeStruct((members, members), BF16),
        ),
        in_specs=[smem, vmem, vmem],
        out_specs=(vmem, vmem),
        scratch_shapes=[pltpu.VMEM((windows, members, members), BF16)] * 2
        + [pltpu.VMEM((windows, members, members), F32)]
        + [pltpu.VMEM((windows, half, half), F32)] * 3,
        compiler_params=pltpu.CompilerParams(vmem_limit_bytes=16 * MIB),
        cost_estimate=pl.CostEstimate(flops=4 * 10**9, bytes_accessed=2 * MIB, transcendentals=0),
        name="transforms",
    )(inflation, gathered, gathered_weights)
    devices = lax.axis_size("tm")
    hops = pltpu.SemaphoreType.DMA((devices // 2, 3))
    weight_mats = pl.pallas_call(
        lambda *refs: suffix_kernel("tm", devices, *refs),
        out_shape=jax.ShapeDtypeStruct((windows, members, members), BF16),
        in_specs=[vmem, vmem],
        out_specs=vmem,
        scratch_shapes=[
            pltpu.VMEM((windows, members, members), F32),
            pltpu.VMEM((members, members), BF16),
            pltpu.VMEM((members, members), BF16),
            pltpu.VMEM((devices // 2, members, members), BF16),
            pltpu.SemaphoreType.DMA((2,)),
        ]
        + [hops] * 4,
        compiler_params=pltpu.CompilerParams(
            collective_id=1, has_side_effects=True, vmem_limit_bytes=8 * MIB
        ),
        cost_estimate=pl.CostEstimate(flops=2 * 10**9, bytes_accessed=MIB, transcendentals=0),
        name="suffix",
    )(own, partial)
    flat = anomalies.reshape(windows, fields * cell_width, members)
    tile = min(512, cell_width)
    result = pl.pallas_call(
        apply_kernel,
        out_shape=jax.ShapeDtypeStruct(flat.shape, BF16),
        in_specs=[vmem, vmem],
        out_specs=hbm,
        scratch_shapes=[
            pltpu.VMEM((windows, fields * cell_width // tile, tile, members), BF16),
            pltpu.SemaphoreType.DMA((windows, fields * cell_width // tile)),
        ],
        compiler_params=pltpu.CompilerParams(vmem_limit_bytes=16 * MIB),
        name="apply",
    )(flat, weight_mats)
    return result.reshape(anomalies.shape)


def solution(mesh):
    placed = (
        P("tm", None, "cell", None),
        P("tm", "cell"),
        P("tm", "cell"),
        P("tm", "cell"),
        P("tm"),
    )
    return jax.shard_map(
        local, mesh=mesh, in_specs=placed, out_specs=P("tm", None, "cell", None), check_vma=False
    )
```
